256 devices in a mesh: member: 4 (over y, x), wave: 64 (over z, core).
Axes of the slice: x: 2, y: 2, z: 32, core: 2. Of those that a mesh axis runs over, the one named last changes fastest.
The devices are a block of a 4x8x32 slice.
Arguments:
- vorticity: bfloat16 [5120, 32, 1280], P(('member', 'wave')), parts along dimension 0, may hold values from -6 to 6
- divergence: bfloat16 [5120, 32, 1280], P(('member', 'wave')), parts along dimension 0, may hold values from -6 to 6
- legendre: bfloat16 [1280, 64, 1280], P('wave'), may hold values from -0.0068359375 to 0.0068359375
- wave_of_slot: int32 [1280], replicated, may hold values from 0 to 1279, as said below
- cycle_points: int32 [64], P('wave'), may hold values from 20 to 5136, as said below
- cos_squared: float32 [64], P('wave'), may hold values from 0.25 to 1
Outputs:
- grid: bfloat16 [256, 96, 5136], P(('member', 'wave')), parts along dimension 0
The draws below stay inside these ranges and needn't reach their ends.
There are 4 independent parts, one for each index of `member`. The reference program is written for one: setup_inputs(seed, part) draws one part's arguments, and reference() takes and returns one part's arrays. A program takes and returns all parts, laid end to end along the dimension named above; an argument that names none is the same for every part. Nothing has to cross between parts.
Inputs may be any that keep to these rules, and one draw needn't show every extreme that they name: `wave_of_slot`: each wavenumber appears in exactly one slot. `cycle_points`: every count is a multiple of 4; some cycle has 5136 points.
All inputs are finite; a program needn't handle non-finite values.
Results may differ from the reference program's by a relative error of at most 0.0063.
Values may be sent and summed in bfloat16 or wider, within the bound.
A program may use at most 128 MiB of HBM per device.

```python
import jax
import jax.numpy as jnp
from jax import lax

NWAVE = 1280
LEV = 16
NLON = 5136
NLAT_WIN = 64


def draw_wave_of_slot(key, part):
    return jax.random.permutation(key, NWAVE).astype(jnp.int32)


def draw_cycle_points(key, part):
    key_steps, key_place = jax.random.split(key)
    counts = jax.random.randint(key_steps, (NLAT_WIN,), 0, (NLON - 20) // 4 + 1, dtype=jnp.int32)
    widest = jax.random.randint(key_place, (), 0, NLAT_WIN, dtype=jnp.int32)
    based = 20 + 4 * counts
    return jnp.where(jnp.arange(NLAT_WIN, dtype=jnp.int32) == widest, NLON, based).astype(jnp.int32)


def level_of(key, extent, cuts, least, largest):
    gain, own = 1.0, jax.random.fold_in(key, 6)
    for dim, shards_of in cuts:
        draws = jnp.exp(jax.random.uniform(jax.random.fold_in(own, dim), (shards_of,), jnp.float32, least / len(cuts), largest / len(cuts)))
        gain = gain * jnp.repeat(draws, extent[dim] // shards_of).reshape([-1 if axis == dim else 1 for axis in range(len(extent))])
    return gain


def noise(own_key, extent, spread, bound, cuts=(), held_as=jnp.bfloat16):
    result = jax.random.normal(own_key, extent, jnp.float32) * spread
    if len(cuts) > 0:
        result = level_of(own_key, extent, cuts, -0.22, 0.18) * result
    return jnp.clip(result, min=-bound, max=bound).astype(held_as)


def setup_inputs(seed: int = 0, part: int = 0) -> dict:
    key_of = jax.random.split(jax.random.key(seed), 7)
    own_keys = jax.random.split(jax.random.fold_in(key_of[6], part), 7)
    vorticity = noise(own_keys[0], (NWAVE, 2 * LEV, NWAVE), 1.0, 6.0, ((0, 64),))
    divergence = noise(own_keys[1], (NWAVE, 2 * LEV, NWAVE), 1.0, 6.0, ((0, 64),))
    legendre = noise(key_of[2], (NWAVE, NLAT_WIN, NWAVE), (NWAVE * NWAVE // 2) ** -0.5, 0.0068359375, ((0, 64),))
    wave_of_slot = draw_wave_of_slot(jax.random.fold_in(key_of[6], 71), part)
    cycle_points = draw_cycle_points(jax.random.fold_in(key_of[6], 71), part)
    cos_squared = jnp.clip(0.25 + 0.75 * jax.random.uniform(key_of[5], (NLAT_WIN,), jnp.float32) ** level_of(key_of[5], (NLAT_WIN,), ((0, 64),), -0.2, 0.2), 0.25, 1.0)
    return dict(vorticity=vorticity, divergence=divergence, legendre=legendre, wave_of_slot=wave_of_slot, cycle_points=cycle_points, cos_squared=cos_squared)


def spectral_fields(zeta_in, delta_in, waves):
    columns = zeta_in.shape[-1]
    levels = zeta_in.shape[1] // 2
    degree = waves[:, None] + jnp.arange(columns, dtype=jnp.int32)[None, :]
    living = degree < NWAVE
    positive = living & (degree > 0)
    wave_f = waves.astype(jnp.float32)[:, None]
    degree_f = degree.astype(jnp.float32)
    radius = NWAVE / 4.0
    inverse = jnp.where(positive, -radius / jnp.maximum(degree_f * (degree_f + 1.0), 1.0), 0.0)
    quotient = jnp.maximum(degree_f * degree_f - wave_f * wave_f, 0.0) / jnp.maximum(4.0 * degree_f * degree_f - 1.0, 1.0)
    coupling = jnp.where(positive, jnp.sqrt(quotient), 0.0)
    coupling_next = jnp.concatenate([coupling[:, 1:], jnp.zeros_like(coupling[:, :1])], axis=1)
    upper_coef = ((degree_f + 2.0) * coupling_next)[:, None, :]
    lower_coef = ((degree_f - 1.0) * coupling)[:, None, :]
    live_mask = living.astype(jnp.float32)[:, None, :]
    zeta = zeta_in.astype(jnp.float32) * live_mask
    delta = delta_in.astype(jnp.float32) * live_mask
    stream = zeta * inverse[:, None, :]
    potential = delta * inverse[:, None, :]

    def meridional(values):
        shifted_up = jnp.concatenate([values[..., 1:], jnp.zeros_like(values[..., :1])], axis=-1)
        shifted_down = jnp.concatenate([jnp.zeros_like(values[..., :1]), values[..., :-1]], axis=-1)
        return (upper_coef * shifted_up - lower_coef * shifted_down) * live_mask
    stream_h = meridional(stream)
    potential_h = meridional(potential)
    wave_three = waves.astype(jnp.float32)[:, None, None]
    u_real = -wave_three * potential[:, levels:] - stream_h[:, :levels]
    u_imag = wave_three * potential[:, :levels] - stream_h[:, levels:]
    v_real = -wave_three * stream[:, levels:] + potential_h[:, :levels]
    v_imag = wave_three * stream[:, :levels] + potential_h[:, levels:]
    return jnp.concatenate([u_real, u_imag, v_real, v_imag, zeta, delta], axis=1).astype(jnp.bfloat16)

def derive(fourier, waves, cosine_sq):
    cycles, slots, columns = fourier.shape
    levels = columns // 8
    groups = fourier.reshape(cycles, slots, 4, 2, levels)
    wind_u = groups[:, :, 0]
    wind_v = groups[:, :, 1]
    zeta_f = groups[:, :, 2]
    delta_f = groups[:, :, 3]
    scale = (waves.astype(jnp.float32) / (NWAVE / 4.0))[None, :, None]
    u_lon = jnp.stack([-scale * wind_u[:, :, 1], scale * wind_u[:, :, 0]], axis=2)
    v_lon = jnp.stack([-scale * wind_v[:, :, 1], scale * wind_v[:, :, 0]], axis=2)
    factor = cosine_sq[:, None, None, None]
    u_lat = v_lon / factor - zeta_f
    v_lat = delta_f - u_lon / factor
    stacked = jnp.stack([wind_u, wind_v, u_lon, v_lon, u_lat, v_lat], axis=2)
    return stacked.reshape(cycles, slots, 12 * levels)

def cycle_basis(waves, points):
    positions = jnp.arange(NLON, dtype=jnp.int32)
    phase = waves[:, None] * positions[None, :] % points
    theta = 2.0 * jnp.pi / points.astype(jnp.float32) * phase.astype(jnp.float32)
    keeping = (2 * waves[:, None] < points) & (positions[None, :] < points)
    weight = jnp.where(waves == 0, 1.0, 2.0)[:, None]
    cosine = jnp.where(keeping, weight * jnp.cos(theta), 0.0)
    sine = jnp.where(keeping, -weight * jnp.sin(theta), 0.0)
    return jnp.stack([cosine, sine]).astype(jnp.bfloat16)

def reference(vorticity, divergence, legendre, wave_of_slot, cycle_points, cos_squared):
    blocks = NWAVE // 16

    def block_fourier(item):
        zeta_in, delta_in, values, waves = item
        spec = spectral_fields(zeta_in, delta_in, waves)
        return jnp.einsum('sck,slk->lsc', spec.astype(jnp.float32), values.astype(jnp.float32))
    items = (vorticity.reshape(blocks, 16, 2 * LEV, NWAVE), divergence.reshape(blocks, 16, 2 * LEV, NWAVE), legendre.reshape(blocks, 16, NLAT_WIN, NWAVE), wave_of_slot.reshape(blocks, 16))
    mapped = lax.map(block_fourier, items)
    fourier = jnp.transpose(mapped, (1, 0, 2, 3)).reshape(NLAT_WIN, NWAVE, 8 * LEV)
    fields = derive(fourier, wave_of_slot, cos_squared)

    def one_cycle(item):
        cycle_fields, points = item
        packed = cycle_fields.astype(jnp.bfloat16).reshape(NWAVE, 6, 2, LEV).astype(jnp.float32)
        basis = cycle_basis(wave_of_slot, points).astype(jnp.float32)
        summed = jnp.einsum('sfrl,rsp->flp', packed, basis)
        return summed.reshape(6 * LEV, NLON).astype(jnp.bfloat16)
    return lax.map(one_cycle, (fields, cycle_points))
```

```python
import functools

import jax
import jax.numpy as jnp
from jax import lax
from jax.experimental import pallas as pl
from jax.experimental.pallas import tpu as pltpu
from jax.sharding import PartitionSpec as P

NLON = 5136
MESH = pl.DeviceIdType.MESH
F32 = jnp.float32
BF16 = jnp.bfloat16
LANES = 128
NBLOCK = 768
NPAD = -(-NLON // NBLOCK) * NBLOCK
HEAD = 16
GROUP = 16
NT = (((1,), (1,)), ((), ()))


def partner(r, z, c, chips, sign):
    q = r // 2
    x = r % 2
    d = jnp.where(q % 2 == 1, (q + 1) // 2, chips - q // 2)
    chip = (z + 2 * chips + sign * d) % chips
    return chip * 2 + (c + x) % 2


def kernel(
    vort, div, leg, wave, points, cosq, out,
    spec, legv, mown, coef_a, coef_b, coef_c, res,
    send_a, send_b, recv_a, recv_b, mb, basis, fields, acc,
    in_sem, ssem, rsem_a, rsem_b,
    *, n, nwave,
):
    w = lax.axis_index("wave")
    z = w // 2
    c = w % 2
    chips = n // 2
    slots = vort.shape[0]
    rows = vort.shape[1]
    half = rows // 2
    tail = slots - HEAD
    radius = nwave / 4.0
    steps = in_sem.shape[0]
    per = slots // steps
    groups = n // GROUP
    ka = GROUP * HEAD

    def loads(g):
        at = pl.ds(g * per, per)
        return (
            pltpu.make_async_copy(vort.at[at], spec.at[at, pl.ds(2 * rows, rows)], in_sem.at[g, 0]),
            pltpu.make_async_copy(div.at[at], spec.at[at, pl.ds(3 * rows, rows)], in_sem.at[g, 1]),
            pltpu.make_async_copy(leg.at[at], legv.at[at], in_sem.at[g, 2]),
        )

    for g in range(steps):
        for copy in loads(g):
            copy.start()

    barrier = pltpu.get_barrier_semaphore()

    def greet(r, carry):
        pl.semaphore_signal(
            barrier, inc=1, device_id={"wave": partner(r, z, c, chips, -1)}, device_id_type=MESH
        )
        return carry

    lax.fori_loop(1, n, greet, 0)

    mown[...] = jnp.zeros_like(mown)
    for s in range(slots):
        mown[s : s + 1, :] = jnp.full((1, LANES), wave[w * slots + s].astype(F32), F32)
    m_own = mown[...]
    lane = lax.broadcasted_iota(jnp.int32, m_own.shape, 1).astype(F32)

    def coupled(deg):
        quotient = jnp.maximum(deg * deg - m_own * m_own, 0.0) / (4.0 * deg * deg - 1.0)
        return -radius * jnp.sqrt(quotient) / deg

    for j in range(nwave // LANES):
        cols = slice(j * LANES, (j + 1) * LANES)
        deg = m_own + (lane + float(j * LANES))
        safe = jnp.maximum(deg, 1.0)
        live = deg < float(nwave)
        coef_a[:, cols] = jnp.where(live & (deg >= 1.0), -radius * m_own / (safe * (safe + 1.0)), 0.0)
        coef_b[:, cols] = jnp.where(deg + 1.0 < float(nwave), coupled(deg + 1.0), 0.0)
        coef_c[:, cols] = jnp.where(live & (deg >= 2.0), coupled(safe), 0.0)

    lane16 = lax.broadcasted_iota(jnp.int32, (16, nwave), 1)

    def one_slot(s, carry):
        m = wave[w * slots + s]
        a = coef_a[pl.ds(s, 1), :]
        b = coef_b[pl.ds(s, 1), :]
        cc = coef_c[pl.ds(s, 1), :]
        parts = []
        for i in range(4):
            x = spec[s, pl.ds(2 * rows + half * i, half), :].astype(F32)
            up = pltpu.roll(x, nwave - 1, 1)
            down = pltpu.roll(x, 1, 1)
            parts.append((x * a, up * b - down * cc))
        (zr, hzr), (zi, hzi), (dr, hdr), (di, hdi) = parts
        spec[s, pl.ds(0, half), :] = (-di - hzr).astype(BF16)
        spec[s, pl.ds(half, half), :] = (dr - hzi).astype(BF16)
        spec[s, pl.ds(2 * half, half), :] = (-zi + hdr).astype(BF16)
        spec[s, pl.ds(3 * half, half), :] = (zr + hdi).astype(BF16)
        mask = jnp.where(lane16 < nwave - m, 1.0, 0.0).astype(BF16)
        values = legv[s]
        masked = jnp.concatenate([values[16 * i : 16 * i + 16] * mask for i in range(n // 16)], axis=0)
        res[pl.ds(pl.multiple_of(s * n, n), n), :] = lax.dot_general(
            masked, spec[s], NT, preferred_element_type=F32
        )
        return carry

    for g in range(steps):
        for copy in loads(g):
            copy.wait()
        lax.fori_loop(g * per, (g + 1) * per, one_slot, 0)

    def pack(r, carry):
        dst = partner(r, z, c, chips, -1)
        send_a[r] = res[pl.ds(dst, HEAD, stride=n), :].astype(BF16)
        send_b[r] = res[pl.ds(HEAD * n + dst, tail, stride=n), :].astype(BF16)
        return carry

    lax.fori_loop(0, n, pack, 0)
    recv_a[0] = send_a[0]
    recv_b[0] = send_b[0]

    pl.semaphore_wait(barrier, n - 1)

    def post_b(j, carry):
        r = n - 1 - j
        pltpu.make_async_remote_copy(
            src_ref=send_b.at[r], dst_ref=recv_b.at[r], send_sem=ssem.at[1], recv_sem=rsem_b,
            device_id={"wave": partner(r, z, c, chips, -1)}, device_id_type=MESH,
        ).start()
        return carry

    def post_a(j, carry):
        r = n - 1 - j
        pltpu.make_async_remote_copy(
            src_ref=send_a.at[r], dst_ref=recv_a.at[r], send_sem=ssem.at[0], recv_sem=rsem_a.at[r // GROUP],
            device_id={"wave": partner(r, z, c, chips, -1)}, device_id_type=MESH,
        ).start()
        return carry

    lax.fori_loop(0, n - 1, post_b, 0)
    lax.fori_loop(0, n - 1, post_a, 0)

    def place(r, carry):
        base = partner(r, z, c, chips, 1) * slots
        for s in range(HEAD):
            mb[pl.ds(r * HEAD + s, 1), :] = jnp.full((1, LANES), wave[base + s].astype(F32), F32)
        for s in range(tail):
            mb[pl.ds(n * HEAD + r * tail + s, 1), :] = jnp.full(
                (1, LANES), wave[base + HEAD + s].astype(F32), F32
            )
        return carry

    lax.fori_loop(0, n, place, 0)

    count = points[0].astype(F32)
    pv = jnp.full((1, LANES), count, F32)
    ip = 1.0 / pv

    def turn(x):
        t = (x - jnp.floor(x * ip + 0.5) * pv) * ip
        u = t * 3.14159265358979
        v = u * u
        sn = u * (1.0 + v * (-1.0 / 6 + v * (1.0 / 120 + v * (-1.0 / 5040 + v * (1.0 / 362880 - v / 39916800)))))
        cs = 1.0 + v * (
            -0.5 + v * (1.0 / 24 + v * (-1.0 / 720 + v * (1.0 / 40320 + v * (-1.0 / 3628800 + v / 479001600))))
        )
        return 1.0 - 2.0 * sn * sn, 2.0 * sn * cs

    span = 32

    def make_basis(i, carry):
        m = mb[pl.ds(pl.multiple_of(i * span, span), span), :]
        pos = lax.broadcasted_iota(jnp.int32, m.shape, 1).astype(F32)
        c0, s0 = turn(m * pos)
        cr, sr = turn(m * float(LANES))
        weight = jnp.where(m == 0.0, 1.0, 2.0)
        weight = jnp.where(2.0 * m < pv, weight, 0.0)
        cv = weight * c0
        sv = -weight * s0
        g = i // (ka // span)
        at = pl.multiple_of((i % (ka // span)) * span, span)
        for j in range(NPAD // LANES):
            cols = slice(j * LANES, (j + 1) * LANES)
            basis[g, pl.ds(at, span), cols] = cv.astype(BF16)
            basis[g, pl.ds(at + ka, span), cols] = sv.astype(BF16)
            cv, sv = cv * cr + sv * sr, sv * cr - cv * sr
        return carry

    lax.fori_loop(0, mb.shape[0] // span, make_basis, 0)

    eye = (
        lax.broadcasted_iota(jnp.int32, (LANES, LANES), 0) == lax.broadcasted_iota(jnp.int32, (LANES, LANES), 1)
    ).astype(F32).astype(BF16)
    first = (lax.broadcasted_iota(jnp.int32, (8, LANES), 1) == 0).astype(F32)
    inv_c = 1.0 / jnp.full((1, ka), cosq[0], F32)

    def derive(g, arrived):
        mrow = lax.dot_general(
            first, mb[pl.ds(g * ka, ka), :], NT, precision=lax.Precision.HIGHEST, preferred_element_type=F32
        )
        q = mrow[0:1] / radius
        x = lax.dot_general(eye, arrived, NT, preferred_element_type=F32)
        ur, ui, vr, vi, zr, zi, dr, di = (x[half * i : half * (i + 1)] for i in range(8))
        for side, (u, v, ul, vl, zt, dl) in enumerate(
            ((ur, vr, -q * ui, -q * vi, zr, dr), (ui, vi, q * ur, q * vr, zi, di))
        ):
            parts = (u, v, ul, vl, vl * inv_c - zt, dl - ul * inv_c)
            for f, part in enumerate(parts):
                fields[half * f : half * (f + 1), ka * side : ka * (side + 1)] = part.astype(BF16)

    def accumulate(g, opening):
        def column(j, carry):
            at = pl.ds(pl.multiple_of(j * NBLOCK, NBLOCK), NBLOCK)
            new = jnp.dot(fields[...], basis[g, :, at], preferred_element_type=F32)
            acc[:, at] = new if opening else acc[:, at] + new
            return carry

        lax.fori_loop(0, NPAD // NBLOCK, column, 0)

    pltpu.make_async_copy(recv_b.at[pl.ds(1, n - 1)], recv_b.at[pl.ds(1, n - 1)], rsem_b).wait()
    derive(groups, recv_b[...].reshape(n * tail, LANES))
    accumulate(groups, True)
    for g in range(groups - 1, -1, -1):
        at = pl.ds(1, GROUP - 1) if g == 0 else pl.ds(g * GROUP, GROUP)
        pltpu.make_async_copy(recv_a.at[at], recv_a.at[at], rsem_a.at[g]).wait()
        derive(g, recv_a[pl.ds(g * GROUP, GROUP)].reshape(ka, LANES))
        if g > 0:
            accumulate(g, False)

    for j in range(NPAD // NBLOCK):
        lo = j * NBLOCK
        hi = min(lo + NBLOCK, NLON)
        new = jnp.dot(fields[...], basis[0, :, lo : lo + NBLOCK], preferred_element_type=F32)
        total = acc[:, lo : lo + NBLOCK] + new
        pos = lax.broadcasted_iota(jnp.int32, total.shape, 1) + lo
        out[0, :, lo:hi] = jnp.where(pos < points[0], total, 0.0).astype(BF16)[:, : hi - lo]

    pltpu.make_async_copy(send_a.at[pl.ds(1, n - 1)], send_a.at[pl.ds(1, n - 1)], ssem.at[0]).wait()
    pltpu.make_async_copy(send_b.at[pl.ds(1, n - 1)], send_b.at[pl.ds(1, n - 1)], ssem.at[1]).wait()


def solution(mesh):
    n = mesh.shape["wave"]

    def body(vort, div, leg, wave, points, cosq):
        slots, rows, nwave = vort.shape
        tail = slots - HEAD
        fields = 12 * rows // 4
        hbm = pl.BlockSpec(memory_space=pl.ANY)
        smem = pl.BlockSpec(memory_space=pltpu.SMEM)
        groups = n // GROUP
        own = -(-slots // 8) * 8
        return pl.pallas_call(
            functools.partial(kernel, n=n, nwave=nwave),
            out_shape=jax.ShapeDtypeStruct((1, fields, NLON), BF16),
            in_specs=[hbm, hbm, hbm, smem, smem, smem],
            out_specs=pl.BlockSpec(memory_space=pltpu.VMEM),
            scratch_shapes=[
                pltpu.VMEM((slots, 4 * rows, nwave), BF16),
                pltpu.VMEM((slots, n, nwave), BF16),
                pltpu.VMEM((own, LANES), F32),
                pltpu.VMEM((own, nwave), F32),
                pltpu.VMEM((own, nwave), F32),
                pltpu.VMEM((own, nwave), F32),
                pltpu.VMEM((slots * n, LANES), F32),
                pltpu.VMEM((n, HEAD, LANES), BF16),
                pltpu.VMEM((n, tail, LANES), BF16),
                pltpu.VMEM((n, HEAD, LANES), BF16),
                pltpu.VMEM((n, tail, LANES), BF16),
                pltpu.VMEM((n * slots, LANES), F32),
                pltpu.VMEM((groups + 1, 2 * GROUP * HEAD, NPAD), BF16),
                pltpu.VMEM((fields, 2 * GROUP * HEAD), BF16),
                pltpu.VMEM((fields, NPAD), F32),
                pltpu.SemaphoreType.DMA((4, 3)),
                pltpu.SemaphoreType.DMA((2,)),
                pltpu.SemaphoreType.DMA((groups,)),
                pltpu.SemaphoreType.DMA,
            ],
            compiler_params=pltpu.CompilerParams(
                collective_id=0, has_side_effects=True, vmem_limit_bytes=60 * 1024 * 1024
            ),
            name="synthesis",
        )(vort, div, leg, wave, points, cosq)

    both = P(("member", "wave"), None, None)
    return jax.shard_map(
        body,
        mesh=mesh,
        in_specs=(both, both, P("wave", None, None), P(None), P("wave"), P("wave")),
        out_specs=both,
        check_vma=False,
    )
```

```python
import functools

import jax
import jax.numpy as jnp
from jax import lax
from jax.experimental import pallas as pl
from jax.experimental.pallas import tpu as pltpu
from jax.sharding import PartitionSpec as P

NLON = 5136
MESH = pl.DeviceIdType.MESH
F32 = jnp.float32
BF16 = jnp.bfloat16
LANES = 128
NBLOCK = 768
NPAD = -(-NLON // NBLOCK) * NBLOCK
HEAD = 16
GROUP = 16
NT = (((1,), (1,)), ((), ()))


def wrapped(chip, chips):
    chip = jnp.where(chip >= chips, chip - chips, chip)
    return jnp.where(chip < 0, chip + chips, chip)


def kernel(
    vort, div, leg, wave, points, cosq, out,
    spec, legv, mown, coef_a, coef_b, coef_c, res,
    send_a, send_b, recv_a, recv_b, mb, basis, qrow, fields, acc,
    in_sem, ssem, rsem_a, rsem_b, far,
    *, n, nwave,
):
    w = lax.axis_index("wave")
    z = w // 2
    c = w % 2
    chips = n // 2
    slots = vort.shape[0]
    rows = vort.shape[1]
    half = rows // 2
    tail = slots - HEAD
    radius = nwave / 4.0
    steps = in_sem.shape[0]
    per = slots // steps
    groups = n // GROUP
    ka = GROUP * HEAD

    def loads(g):
        at = pl.ds(g * per, per)
        return (
            pltpu.make_async_copy(vort.at[at], spec.at[at, pl.ds(2 * rows, rows)], in_sem.at[g, 0]),
            pltpu.make_async_copy(div.at[at], spec.at[at, pl.ds(3 * rows, rows)], in_sem.at[g, 1]),
            pltpu.make_async_copy(leg.at[at], legv.at[at], in_sem.at[g, 2]),
        )

    for g in (steps - 1, *range(steps - 1)):
        for copy in loads(g):
            copy.start()

    barrier = pltpu.get_barrier_semaphore()
    near = chips // 4

    def hello(dev):
        pl.semaphore_signal(barrier, inc=1, device_id={"wave": dev}, device_id_type=MESH)

    hello(2 * z + 1 - c)

    def greet(k, carry):
        for chip in (wrapped(z - k, chips), wrapped(z + k, chips)):
            hello(2 * chip)
            hello(2 * chip + 1)
        return carry

    lax.fori_loop(1, near + 1, greet, 0)

    mown[...] = jnp.zeros_like(mown)
    for s in range(slots):
        mown[s : s + 1, :] = jnp.full((1, LANES), wave[w * slots + s].astype(F32), F32)
    m_own = mown[...]
    lane = lax.broadcasted_iota(jnp.int32, m_own.shape, 1).astype(F32)

    def coupled(deg):
        quotient = jnp.maximum(deg * deg - m_own * m_own, 0.0) / (4.0 * deg * deg - 1.0)
        return -radius * jnp.sqrt(quotient) / deg

    for j in range(nwave // LANES):
        cols = slice(j * LANES, (j + 1) * LANES)
        deg = m_own + (lane + float(j * LANES))
        safe = jnp.maximum(deg, 1.0)
        live = deg < float(nwave)
        coef_a[:, cols] = jnp.where(live & (deg >= 1.0), -radius * m_own / (safe * (safe + 1.0)), 0.0)
        coef_b[:, cols] = jnp.where(deg + 1.0 < float(nwave), coupled(deg + 1.0), 0.0)
        coef_c[:, cols] = jnp.where(live & (deg >= 2.0), coupled(safe), 0.0)

    lane16 = lax.broadcasted_iota(jnp.int32, (16, nwave), 1)
    pitch = n + 8

    def one_slot(s):
        m = wave[w * slots + s]
        a = coef_a[pl.ds(s, 1), :]
        b = coef_b[pl.ds(s, 1), :]
        cc = coef_c[pl.ds(s, 1), :]
        parts = []
        for i in range(4):
            x = spec[s, pl.ds(2 * rows + half * i, half), :].astype(F32)
            up = pltpu.roll(x, nwave - 1, 1)
            down = pltpu.roll(x, 1, 1)
            parts.append((x * a, up * b - down * cc))
        (zr, hzr), (zi, hzi), (dr, hdr), (di, hdi) = parts
        spec[s, pl.ds(0, half), :] = (-di - hzr).astype(BF16)
        spec[s, pl.ds(half, half), :] = (dr - hzi).astype(BF16)
        spec[s, pl.ds(2 * half, half), :] = (-zi + hdr).astype(BF16)
        spec[s, pl.ds(3 * half, half), :] = (zr + hdi).astype(BF16)
        mask = jnp.where(lane16 < nwave - m, 1.0, 0.0).astype(BF16)
        values = legv[s]
        masked = jnp.concatenate([values[16 * i : 16 * i + 16] * mask for i in range(n // 16)], axis=0)
        res[pl.ds(pl.multiple_of(s * pitch, 8), n), :] = lax.dot_general(
            masked, spec[s], NT, preferred_element_type=F32
        )

    def quad(g, carry):
        for copy in loads(g):
            copy.wait()
        for u in range(per):
            one_slot(g * per + u)
        return carry

    def post(src, dst, rsem, ssem, r, dev):
        pltpu.make_async_remote_copy(
            src_ref=src.at[dev], dst_ref=dst.at[r], send_sem=ssem, recv_sem=rsem,
            device_id={"wave": dev}, device_id_type=MESH,
        ).start()

    def post_b(r, dev):
        post(send_b, recv_b, rsem_b, ssem.at[1], r, dev)

    def post_a(r, dev):
        post(send_a, recv_a, rsem_a.at[r // GROUP], ssem.at[0], r, dev)

    def outward(send, high, low):
        def trip(j, carry):
            k = high - j
            for q, chip in ((2 * k - 1, wrapped(z - k, chips)), (2 * k, wrapped(z + k, chips))):
                send(2 * q, 2 * chip + c)
                send(2 * q + 1, 2 * chip + 1 - c)
            return carry

        lax.fori_loop(0, high - low + 1, trip, 0)

    def across(send):
        chip = wrapped(z + chips // 2, chips)
        send(2 * (chips - 1), 2 * chip + c)
        send(2 * (chips - 1) + 1, 2 * chip + 1 - c)

    quad(steps - 1, 0)
    for dev in range(n):
        send_b[dev] = res[pl.ds(HEAD * pitch + dev, tail, stride=pitch), :].astype(BF16)
    recv_b[0] = send_b[w]
    lax.fori_loop(0, steps - 1, quad, 0)
    for dev in range(n):
        send_a[dev] = res[pl.ds(dev, HEAD, stride=pitch), :].astype(BF16)
    recv_a[0] = send_a[w]

    pl.semaphore_wait(barrier, 2 * (2 * near + 1) - 1)
    for chip in (wrapped(z - near, chips), wrapped(z + near, chips)):
        pl.semaphore_signal(far, inc=1, device_id={"wave": 2 * chip + c}, device_id_type=MESH)
    outward(post_b, near, 1)
    outward(post_a, near, near - 1)

    def rows_of(r, dev):
        base = dev * slots
        for s in range(HEAD):
            mb[pl.ds(r * HEAD + s, 1), :] = jnp.full((1, LANES), wave[base + s].astype(F32), F32)
        for s in range(tail):
            mb[pl.ds(n * HEAD + r * tail + s, 1), :] = jnp.full(
                (1, LANES), wave[base + HEAD + s].astype(F32), F32
            )

    def place(q, carry):
        d = jnp.where(q % 2 == 1, (q + 1) // 2, -(q // 2))
        chip = wrapped(z + d, chips)
        rows_of(2 * q, 2 * chip + c)
        rows_of(2 * q + 1, 2 * chip + 1 - c)
        return carry

    lax.fori_loop(0, chips, place, 0)

    count = points[0].astype(F32)
    pv = jnp.full((1, LANES), count, F32)
    ip = 1.0 / pv

    def turn(x):
        t = (x - jnp.floor(x * ip + 0.5) * pv) * ip
        u = t * 3.14159265358979
        v = u * u
        sn = u * (1.0 + v * (-1.0 / 6 + v * (1.0 / 120 + v * (-1.0 / 5040 + v * (1.0 / 362880 - v / 39916800)))))
        cs = 1.0 + v * (
            -0.5 + v * (1.0 / 24 + v * (-1.0 / 720 + v * (1.0 / 40320 + v * (-1.0 / 3628800 + v / 479001600))))
        )
        return 1.0 - 2.0 * sn * sn, 2.0 * sn * cs

    span = 32

    def make_basis(i, carry):
        m = mb[pl.ds(pl.multiple_of(i * span, span), span), :]
        pos = lax.broadcasted_iota(jnp.int32, m.shape, 1).astype(F32)
        c0, s0 = turn(m * pos)
        cr, sr = turn(m * float(LANES))
        weight = jnp.where(m == 0.0, 1.0, 2.0)
        weight = jnp.where(2.0 * m < pv, weight, 0.0)
        cv = weight * c0
        sv = -weight * s0
        g = i // (ka // span)
        at = pl.multiple_of((i % (ka // span)) * span, span)
        for j in range(NPAD // LANES):
            cols = slice(j * LANES, (j + 1) * LANES)
            basis[g, pl.ds(at, span), cols] = cv.astype(BF16)
            basis[g, pl.ds(at + ka, span), cols] = sv.astype(BF16)
            cv, sv = cv * cr + sv * sr, sv * cr - cv * sr
        return carry

    trips = mb.shape[0] // span
    lax.fori_loop(groups * (ka // span), trips, make_basis, 0)

    pl.semaphore_wait(far, 2)
    across(post_b)
    outward(post_b, chips // 2 - 1, near + 1)
    across(post_a)
    outward(post_a, chips // 2 - 1, near + 1)
    outward(post_a, near - 2, 1)
    post_b(1, 2 * z + 1 - c)
    post_a(1, 2 * z + 1 - c)

    lax.fori_loop(0, groups * (ka // span), make_basis, 0)

    eye = (
        lax.broadcasted_iota(jnp.int32, (LANES, LANES), 0) == lax.broadcasted_iota(jnp.int32, (LANES, LANES), 1)
    ).astype(F32).astype(BF16)
    first = (lax.broadcasted_iota(jnp.int32, (8, LANES), 1) == 0).astype(F32)
    inv_c = 1.0 / jnp.full((1, ka), cosq[0], F32)

    for g in range(groups + 1):
        qrow[g] = lax.dot_general(
            first, mb[pl.ds(g * ka, ka), :], NT, precision=lax.Precision.HIGHEST, preferred_element_type=F32
        ) / radius

    def derive(g, arrived):
        q = qrow[g, 0:1, :]
        x = lax.dot_general(eye, arrived, NT, preferred_element_type=F32)
        ur, ui, vr, vi, zr, zi, dr, di = (x[half * i : half * (i + 1)] for i in range(8))
        for side, (u, v, ul, vl, zt, dl) in enumerate(
            ((ur, vr, -q * ui, -q * vi, zr, dr), (ui, vi, q * ur, q * vr, zi, di))
        ):
            parts = (u, v, ul, vl, vl * inv_c - zt, dl - ul * inv_c)
            for f, part in enumerate(parts):
                fields[half * f : half * (f + 1), ka * side : ka * (side + 1)] = part.astype(BF16)

    def accumulate(g, opening):
        def column(j, carry):
            at = pl.ds(pl.multiple_of(j * NBLOCK, NBLOCK), NBLOCK)
            new = jnp.dot(fields[...], basis[g, :, at], preferred_element_type=F32)
            acc[:, at] = new if opening else acc[:, at] + new
            return carry

        lax.fori_loop(0, NPAD // NBLOCK, column, 0)

    pltpu.make_async_copy(recv_b.at[pl.ds(1, n - 1)], recv_b.at[pl.ds(1, n - 1)], rsem_b).wait()
    derive(groups, recv_b[...].reshape(n * tail, LANES))
    accumulate(groups, True)
    for g in range(groups - 1, -1, -1):
        at = pl.ds(1, GROUP - 1) if g == 0 else pl.ds(g * GROUP, GROUP)
        pltpu.make_async_copy(recv_a.at[at], recv_a.at[at], rsem_a.at[g]).wait()
        derive(g, recv_a[pl.ds(g * GROUP, GROUP)].reshape(ka, LANES))
        if g > 0:
            accumulate(g, False)

    for j in range(NPAD // NBLOCK):
        lo = j * NBLOCK
        hi = min(lo + NBLOCK, NLON)
        new = jnp.dot(fields[...], basis[0, :, lo : lo + NBLOCK], preferred_element_type=F32)
        total = acc[:, lo : lo + NBLOCK] + new
        pos = lax.broadcasted_iota(jnp.int32, total.shape, 1) + lo
        out[0, :, lo:hi] = jnp.where(pos < points[0], total, 0.0).astype(BF16)[:, : hi - lo]

    pltpu.make_async_copy(send_a.at[pl.ds(1, n - 1)], send_a.at[pl.ds(1, n - 1)], ssem.at[0]).wait()
    pltpu.make_async_copy(send_b.at[pl.ds(1, n - 1)], send_b.at[pl.ds(1, n - 1)], ssem.at[1]).wait()


def solution(mesh):
    n = mesh.shape["wave"]

    def body(vort, div, leg, wave, points, cosq):
        slots, rows, nwave = vort.shape
        tail = slots - HEAD
        fields = 12 * rows // 4
        hbm = pl.BlockSpec(memory_space=pltpu.MemorySpace.HBM)
        smem = pl.BlockSpec(memory_space=pltpu.SMEM)
        groups = n // GROUP
        own = -(-slots // 8) * 8
        return pl.pallas_call(
            functools.partial(kernel, n=n, nwave=nwave),
            out_shape=jax.ShapeDtypeStruct((1, fields, NLON), BF16),
            in_specs=[hbm, hbm, hbm, smem, smem, smem],
            out_specs=pl.BlockSpec(memory_space=pltpu.VMEM),
            scratch_shapes=[
                pltpu.VMEM((slots, 4 * rows, nwave), BF16),
                pltpu.VMEM((slots, n, nwave), BF16),
                pltpu.VMEM((own, LANES), F32),
                pltpu.VMEM((own, nwave), F32),
                pltpu.VMEM((own, nwave), F32),
                pltpu.VMEM((own, nwave), F32),
                pltpu.VMEM((slots * (n + 8), LANES), F32),
                pltpu.VMEM((n, HEAD, LANES), BF16),
                pltpu.VMEM((n, tail, LANES), BF16),
                pltpu.VMEM((n, HEAD, LANES), BF16),
                pltpu.VMEM((n, tail, LANES), BF16),
                pltpu.VMEM((n * slots, LANES), F32),
                pltpu.VMEM((groups + 1, 2 * GROUP * HEAD, NPAD), BF16),
                pltpu.VMEM((groups + 1, 8, GROUP * HEAD), F32),
                pltpu.VMEM((fields, 2 * GROUP * HEAD), BF16),
                pltpu.VMEM((fields, NPAD), F32),
                pltpu.SemaphoreType.DMA((slots // tail, 3)),
                pltpu.SemaphoreType.DMA((2,)),
                pltpu.SemaphoreType.DMA((groups,)),
                pltpu.SemaphoreType.DMA,
                pltpu.SemaphoreType.REGULAR,
            ],
            compiler_params=pltpu.CompilerParams(
                collective_id=0, has_side_effects=True, vmem_limit_bytes=46 * 1024 * 1024
            ),
            name="synthesis",
        )(*(pltpu.with_memory_space_constraint(v, pltpu.MemorySpace.HBM) for v in (vort, div, leg, wave)), points, cosq)

    both = P(("member", "wave"), None, None)
    return jax.shard_map(
        body,
        mesh=mesh,
        in_specs=(both, both, P("wave", None, None), P(None), P("wave"), P("wave")),
        out_specs=both,
        check_vma=False,
    )
```

```python
import functools

import jax
import jax.numpy as jnp
from jax import lax
from jax.experimental import pallas as pl
from jax.experimental.pallas import tpu as pltpu
from jax.sharding import PartitionSpec as P

NLON = 5136
MESH = pl.DeviceIdType.MESH
F32 = jnp.float32
BF16 = jnp.bfloat16
LANES = 128
NBLOCK = 768
NPAD = -(-NLON // NBLOCK) * NBLOCK
HEAD = 16
GROUP = 16
NT = (((1,), (1,)), ((), ()))


def wrapped(chip, chips):
    chip = jnp.where(chip >= chips, chip - chips, chip)
    return jnp.where(chip < 0, chip + chips, chip)


def kernel(
    vort, div, leg, wave, points, cosq, out,
    spec, legv, mown, coef_a, coef_b, coef_c, res,
    send_a, send_b, recv_a, recv_b, mb, basis, qrow, fields, acc,
    in_sem, ssem, rsem_a, rsem_b, far,
    *, n, nwave,
):
    w = lax.axis_index("wave")
    z = w // 2
    c = w % 2
    chips = n // 2
    slots = vort.shape[0]
    rows = vort.shape[1]
    half = rows // 2
    tail = slots - HEAD
    radius = nwave / 4.0
    steps = in_sem.shape[0]
    per = slots // steps
    groups = n // GROUP
    ka = GROUP * HEAD

    def loads(g):
        at = pl.ds(g * per, per)
        return (
            pltpu.make_async_copy(vort.at[at], spec.at[at, pl.ds(2 * rows, rows)], in_sem.at[g, 0]),
            pltpu.make_async_copy(div.at[at], spec.at[at, pl.ds(3 * rows, rows)], in_sem.at[g, 1]),
            pltpu.make_async_copy(leg.at[at], legv.at[at], in_sem.at[g, 2]),
        )

    for g in (steps - 1, *range(steps - 1)):
        for copy in loads(g):
            copy.start()

    barrier = pltpu.get_barrier_semaphore()
    near = chips // 4

    def hello(dev):
        pl.semaphore_signal(barrier, inc=1, device_id={"wave": dev}, device_id_type=MESH)

    hello(2 * z + 1 - c)

    def greet(k, carry):
        for chip in (wrapped(z - k, chips), wrapped(z + k, chips)):
            hello(2 * chip)
            hello(2 * chip + 1)
        return carry

    lax.fori_loop(1, near + 1, greet, 0)

    mown[...] = jnp.zeros_like(mown)
    for s in range(slots):
        mown[s : s + 1, :] = jnp.full((1, LANES), wave[w * slots + s].astype(F32), F32)
    m_own = mown[...]
    lane = lax.broadcasted_iota(jnp.int32, m_own.shape, 1).astype(F32)

    def coupled(deg):
        quotient = jnp.maximum(deg * deg - m_own * m_own, 0.0) / (4.0 * deg * deg - 1.0)
        return -radius * jnp.sqrt(quotient) / deg

    for j in range(nwave // LANES):
        cols = slice(j * LANES, (j + 1) * LANES)
        deg = m_own + (lane + float(j * LANES))
        safe = jnp.maximum(deg, 1.0)
        live = deg < float(nwave)
        coef_a[:, cols] = jnp.where(live & (deg >= 1.0), -radius * m_own / (safe * (safe + 1.0)), 0.0)
        coef_b[:, cols] = jnp.where(deg + 1.0 < float(nwave), coupled(deg + 1.0), 0.0)
        coef_c[:, cols] = jnp.where(live & (deg >= 2.0), coupled(safe), 0.0)

    lane16 = lax.broadcasted_iota(jnp.int32, (16, nwave), 1)
    pitch = n + 8

    def one_slot(s):
        m = wave[w * slots + s]
        a = coef_a[pl.ds(s, 1), :]
        b = coef_b[pl.ds(s, 1), :]
        cc = coef_c[pl.ds(s, 1), :]
        parts = []
        for i in range(4):
            x = spec[s, pl.ds(2 * rows + half * i, half), :].astype(F32)
            up = pltpu.roll(x, nwave - 1, 1)
            down = pltpu.roll(x, 1, 1)
            parts.append((x * a, up * b - down * cc))
        (zr, hzr), (zi, hzi), (dr, hdr), (di, hdi) = parts
        spec[s, pl.ds(0, half), :] = (-di - hzr).astype(BF16)
        spec[s, pl.ds(half, half), :] = (dr - hzi).astype(BF16)
        spec[s, pl.ds(2 * half, half), :] = (-zi + hdr).astype(BF16)
        spec[s, pl.ds(3 * half, half), :] = (zr + hdi).astype(BF16)
        mask = jnp.where(lane16 < nwave - m, 1.0, 0.0).astype(BF16)
        values = legv[s]
        masked = jnp.concatenate([values[16 * i : 16 * i + 16] * mask for i in range(n // 16)], axis=0)
        res[pl.ds(pl.multiple_of(s * pitch, 8), n), :] = lax.dot_general(
            masked, spec[s], NT, preferred_element_type=F32
        )

    def quad(g, carry):
        for copy in loads(g):
            copy.wait()
        for u in range(per):
            one_slot(g * per + u)
        return carry

    def post(src, dst, rsem, ssem, r, dev):
        pltpu.make_async_remote_copy(
            src_ref=src.at[dev], dst_ref=dst.at[r], send_sem=ssem, recv_sem=rsem,
            device_id={"wave": dev}, device_id_type=MESH,
        ).start()

    def post_b(r, dev):
        post(send_b, recv_b, rsem_b, ssem.at[1], r, dev)

    def post_a(r, dev):
        post(send_a, recv_a, rsem_a.at[r // GROUP], ssem.at[0], r, dev)

    def outward(send, high, low):
        def trip(j, carry):
            k = high - j
            for q, chip in ((2 * k - 1, wrapped(z - k, chips)), (2 * k, wrapped(z + k, chips))):
                send(2 * q, 2 * chip + c)
                send(2 * q + 1, 2 * chip + 1 - c)
            return carry

        lax.fori_loop(0, high - low + 1, trip, 0)

    def across(send):
        chip = wrapped(z + chips // 2, chips)
        send(2 * (chips - 1), 2 * chip + c)
        send(2 * (chips - 1) + 1, 2 * chip + 1 - c)

    quad(steps - 1, 0)
    for dev in range(n):
        send_b[dev] = res[pl.ds(HEAD * pitch + dev, tail, stride=pitch), :].astype(BF16)
    recv_b[0] = send_b[w]
    lax.fori_loop(0, steps - 1, quad, 0)
    for dev in range(n):
        send_a[dev] = res[pl.ds(dev, HEAD, stride=pitch), :].astype(BF16)
    recv_a[0] = send_a[w]

    pl.semaphore_wait(barrier, 2 * (2 * near + 1) - 1)
    for chip in (wrapped(z - near, chips), wrapped(z + near, chips)):
        pl.semaphore_signal(far, inc=1, device_id={"wave": 2 * chip + c}, device_id_type=MESH)
    outward(post_a, near, 1)
    outward(post_b, near, 1)
    post_a(1, 2 * z + 1 - c)
    post_b(1, 2 * z + 1 - c)

    def rows_of(r, dev):
        base = dev * slots
        for s in range(HEAD):
            mb[pl.ds(r * HEAD + s, 1), :] = jnp.full((1, LANES), wave[base + s].astype(F32), F32)
        for s in range(tail):
            mb[pl.ds(n * HEAD + r * tail + s, 1), :] = jnp.full(
                (1, LANES), wave[base + HEAD + s].astype(F32), F32
            )

    def place(q, carry):
        d = jnp.where(q % 2 == 1, (q + 1) // 2, -(q // 2))
        chip = wrapped(z + d, chips)
        rows_of(2 * q, 2 * chip + c)
        rows_of(2 * q + 1, 2 * chip + 1 - c)
        return carry

    lax.fori_loop(0, chips, place, 0)

    count = points[0].astype(F32)
    pv = jnp.full((1, LANES), count, F32)
    ip = 1.0 / pv

    def turn(x):
        t = (x - jnp.floor(x * ip + 0.5) * pv) * ip
        u = t * 3.14159265358979
        v = u * u
        sn = u * (1.0 + v * (-1.0 / 6 + v * (1.0 / 120 + v * (-1.0 / 5040 + v * (1.0 / 362880 - v / 39916800)))))
        cs = 1.0 + v * (
            -0.5 + v * (1.0 / 24 + v * (-1.0 / 720 + v * (1.0 / 40320 + v * (-1.0 / 3628800 + v / 479001600))))
        )
        return 1.0 - 2.0 * sn * sn, 2.0 * sn * cs

    span = 32

    def make_basis(i, carry):
        m = mb[pl.ds(pl.multiple_of(i * span, span), span), :]
        pos = lax.broadcasted_iota(jnp.int32, m.shape, 1).astype(F32)
        c0, s0 = turn(m * pos)
        cr, sr = turn(m * float(LANES))
        weight = jnp.where(m == 0.0, 1.0, 2.0)
        weight = jnp.where(2.0 * m < pv, weight, 0.0)
        cv = weight * c0
        sv = -weight * s0
        g = i // (ka // span)
        at = pl.multiple_of((i % (ka // span)) * span, span)
        for j in range(NPAD // LANES):
            cols = slice(j * LANES, (j + 1) * LANES)
            basis[g, pl.ds(at, span), cols] = cv.astype(BF16)
            basis[g, pl.ds(at + ka, span), cols] = sv.astype(BF16)
            cv, sv = cv * cr + sv * sr, sv * cr - cv * sr
        return carry

    trips = mb.shape[0] // span
    lax.fori_loop(groups * (ka // span), trips, make_basis, 0)

    pl.semaphore_wait(far, 2)
    across(post_a)
    across(post_b)
    outward(post_b, chips // 2 - 1, near + 1)
    outward(post_a, chips // 2 - 1, near + 1)

    lax.fori_loop(0, groups * (ka // span), make_basis, 0)

    eye = (
        lax.broadcasted_iota(jnp.int32, (LANES, LANES), 0) == lax.broadcasted_iota(jnp.int32, (LANES, LANES), 1)
    ).astype(F32).astype(BF16)
    first = (lax.broadcasted_iota(jnp.int32, (8, LANES), 1) == 0).astype(F32)
    inv_c = 1.0 / jnp.full((1, ka), cosq[0], F32)

    for g in range(groups + 1):
        qrow[g] = lax.dot_general(
            first, mb[pl.ds(g * ka, ka), :], NT, precision=lax.Precision.HIGHEST, preferred_element_type=F32
        ) / radius

    def derive(g, arrived):
        q = qrow[g, 0:1, :]
        x = lax.dot_general(eye, arrived, NT, preferred_element_type=F32)
        ur, ui, vr, vi, zr, zi, dr, di = (x[half * i : half * (i + 1)] for i in range(8))
        for side, (u, v, ul, vl, zt, dl) in enumerate(
            ((ur, vr, -q * ui, -q * vi, zr, dr), (ui, vi, q * ur, q * vr, zi, di))
        ):
            parts = (u, v, ul, vl, vl * inv_c - zt, dl - ul * inv_c)
            for f, part in enumerate(parts):
                fields[half * f : half * (f + 1), ka * side : ka * (side + 1)] = part.astype(BF16)

    def accumulate(g, opening):
        def column(j, carry):
            at = pl.ds(pl.multiple_of(j * NBLOCK, NBLOCK), NBLOCK)
            new = jnp.dot(fields[...], basis[g, :, at], preferred_element_type=F32)
            acc[:, at] = new if opening else acc[:, at] + new
            return carry

        lax.fori_loop(0, NPAD // NBLOCK, column, 0)

    def quarter(g):
        at = pl.ds(1, GROUP - 1) if g == 0 else pl.ds(g * GROUP, GROUP)
        pltpu.make_async_copy(recv_a.at[at], recv_a.at[at], rsem_a.at[g]).wait()
        derive(g, recv_a[pl.ds(g * GROUP, GROUP)].reshape(ka, LANES))

    last = groups // 2
    for g in range(last):
        quarter(g)
        accumulate(g, g == 0)
    pltpu.make_async_copy(recv_b.at[pl.ds(1, n - 1)], recv_b.at[pl.ds(1, n - 1)], rsem_b).wait()
    derive(groups, recv_b[...].reshape(n * tail, LANES))
    accumulate(groups, False)
    for g in range(groups - 1, last, -1):
        quarter(g)
        accumulate(g, False)
    quarter(last)

    for j in range(NPAD // NBLOCK):
        lo = j * NBLOCK
        hi = min(lo + NBLOCK, NLON)
        new = jnp.dot(fields[...], basis[last, :, lo : lo + NBLOCK], preferred_element_type=F32)
        total = acc[:, lo : lo + NBLOCK] + new
        pos = lax.broadcasted_iota(jnp.int32, total.shape, 1) + lo
        out[0, :, lo:hi] = jnp.where(pos < points[0], total, 0.0).astype(BF16)[:, : hi - lo]

    pltpu.make_async_copy(send_a.at[pl.ds(1, n - 1)], send_a.at[pl.ds(1, n - 1)], ssem.at[0]).wait()
    pltpu.make_async_copy(send_b.at[pl.ds(1, n - 1)], send_b.at[pl.ds(1, n - 1)], ssem.at[1]).wait()


def solution(mesh):
    n = mesh.shape["wave"]

    def body(vort, div, leg, wave, points, cosq):
        slots, rows, nwave = vort.shape
        tail = slots - HEAD
        fields = 12 * rows // 4
        hbm = pl.BlockSpec(memory_space=pltpu.MemorySpace.HBM)
        smem = pl.BlockSpec(memory_space=pltpu.SMEM)
        groups = n // GROUP
        own = -(-slots // 8) * 8
        return pl.pallas_call(
            functools.partial(kernel, n=n, nwave=nwave),
            out_shape=jax.ShapeDtypeStruct((1, fields, NLON), BF16),
            in_specs=[hbm, hbm, hbm, smem, smem, smem],
            out_specs=pl.BlockSpec(memory_space=pltpu.VMEM),
            scratch_shapes=[
                pltpu.VMEM((slots, 4 * rows, nwave), BF16),
                pltpu.VMEM((slots, n, nwave), BF16),
                pltpu.VMEM((own, LANES), F32),
                pltpu.VMEM((own, nwave), F32),
                pltpu.VMEM((own, nwave), F32),
                pltpu.VMEM((own, nwave), F32),
                pltpu.VMEM((slots * (n + 8), LANES), F32),
                pltpu.VMEM((n, HEAD, LANES), BF16),
                pltpu.VMEM((n, tail, LANES), BF16),
                pltpu.VMEM((n, HEAD, LANES), BF16),
                pltpu.VMEM((n, tail, LANES), BF16),
                pltpu.VMEM((n * slots, LANES), F32),
                pltpu.VMEM((groups + 1, 2 * GROUP * HEAD, NPAD), BF16),
                pltpu.VMEM((groups + 1, 8, GROUP * HEAD), F32),
                pltpu.VMEM((fields, 2 * GROUP * HEAD), BF16),
                pltpu.VMEM((fields, NPAD), F32),
                pltpu.SemaphoreType.DMA((slots // tail, 3)),
                pltpu.SemaphoreType.DMA((2,)),
                pltpu.SemaphoreType.DMA((groups,)),
                pltpu.SemaphoreType.DMA,
                pltpu.SemaphoreType.REGULAR,
            ],
            compiler_params=pltpu.CompilerParams(
                collective_id=0, has_side_effects=True, vmem_limit_bytes=46 * 1024 * 1024
            ),
            name="synthesis",
        )(*(pltpu.with_memory_space_constraint(v, pltpu.MemorySpace.HBM) for v in (vort, div, leg, wave)), points, cosq)

    both = P(("member", "wave"), None, None)
    return jax.shard_map(
        body,
        mesh=mesh,
        in_specs=(both, both, P("wave", None, None), P(None), P("wave"), P("wave")),
        out_specs=both,
        check_vma=False,
    )
```

```python
import functools

import jax
import jax.numpy as jnp
from jax import lax
from jax.experimental import pallas as pl
from jax.experimental.pallas import tpu as pltpu
from jax.sharding import PartitionSpec as P

NLON = 5136
MESH = pl.DeviceIdType.MESH
F32 = jnp.float32
BF16 = jnp.bfloat16
LANES = 128
NBLOCK = 768
NPAD = -(-NLON // NBLOCK) * NBLOCK
HEAD = 16
GROUP = 16
NT = (((1,), (1,)), ((), ()))


def wrapped(chip, chips):
    chip = jnp.where(chip >= chips, chip - chips, chip)
    return jnp.where(chip < 0, chip + chips, chip)


def kernel(
    vort, div, leg, wave_in, points, cosq, out,
    wave,
    spec, legv, mown, coef_a, coef_b, coef_c, res,
    send_a, send_b, recv_a, recv_b, mb, basis, qrow, fields, acc,
    in_sem, small_sem, ssem, rsem_a, rsem_b, far,
    *, n, nwave,
):
    w = lax.axis_index("wave")
    z = w // 2
    c = w % 2
    chips = n // 2
    slots = vort.shape[0]
    rows = vort.shape[1]
    half = rows // 2
    tail = slots - HEAD
    radius = nwave / 4.0
    steps = in_sem.shape[0]
    per = slots // steps
    groups = n // GROUP
    ka = GROUP * HEAD

    def loads(g):
        at = pl.ds(g * per, per)
        return (
            pltpu.make_async_copy(vort.at[at], spec.at[at, pl.ds(2 * rows, rows)], in_sem.at[g, 0]),
            pltpu.make_async_copy(div.at[at], spec.at[at, pl.ds(3 * rows, rows)], in_sem.at[g, 1]),
            pltpu.make_async_copy(leg.at[at], legv.at[at], in_sem.at[g, 2]),
        )

    waves = pltpu.make_async_copy(wave_in, wave, small_sem)
    waves.start()
    for g in (steps - 1, *range(steps - 1)):
        for copy in loads(g):
            copy.start()

    barrier = pltpu.get_barrier_semaphore()
    near = chips // 4

    def hello(dev):
        pl.semaphore_signal(barrier, inc=1, device_id={"wave": dev}, device_id_type=MESH)

    def greet(j, carry):
        k = near - j
        for chip in (wrapped(z - k, chips), wrapped(z + k, chips)):
            hello(2 * chip)
            hello(2 * chip + 1)
        return carry

    lax.fori_loop(0, near, greet, 0)
    hello(2 * z + 1 - c)
    waves.wait()

    mown[...] = jnp.zeros_like(mown)
    for s in range(slots):
        mown[s : s + 1, :] = jnp.full((1, LANES), wave[w * slots + s].astype(F32), F32)
    m_own = mown[...]
    lane = lax.broadcasted_iota(jnp.int32, m_own.shape, 1).astype(F32)

    def coupled(deg):
        quotient = jnp.maximum(deg * deg - m_own * m_own, 0.0) / (4.0 * deg * deg - 1.0)
        return -radius * jnp.sqrt(quotient) / deg

    for j in range(nwave // LANES):
        cols = slice(j * LANES, (j + 1) * LANES)
        deg = m_own + (lane + float(j * LANES))
        safe = jnp.maximum(deg, 1.0)
        live = deg < float(nwave)
        coef_a[:, cols] = jnp.where(live & (deg >= 1.0), -radius * m_own / (safe * (safe + 1.0)), 0.0)
        coef_b[:, cols] = jnp.where(deg + 1.0 < float(nwave), coupled(deg + 1.0), 0.0)
        coef_c[:, cols] = jnp.where(live & (deg >= 2.0), coupled(safe), 0.0)

    lane16 = lax.broadcasted_iota(jnp.int32, (16, nwave), 1)
    pitch = n + 8

    def one_slot(s):
        m = wave[w * slots + s]
        a = coef_a[pl.ds(s, 1), :]
        b = coef_b[pl.ds(s, 1), :]
        cc = coef_c[pl.ds(s, 1), :]
        parts = []
        for i in range(4):
            x = spec[s, pl.ds(2 * rows + half * i, half), :].astype(F32)
            up = pltpu.roll(x, nwave - 1, 1)
            down = pltpu.roll(x, 1, 1)
            parts.append((x * a, up * b - down * cc))
        (zr, hzr), (zi, hzi), (dr, hdr), (di, hdi) = parts
        spec[s, pl.ds(0, half), :] = (-di - hzr).astype(BF16)
        spec[s, pl.ds(half, half), :] = (dr - hzi).astype(BF16)
        spec[s, pl.ds(2 * half, half), :] = (-zi + hdr).astype(BF16)
        spec[s, pl.ds(3 * half, half), :] = (zr + hdi).astype(BF16)
        mask = jnp.where(lane16 < nwave - m, 1.0, 0.0).astype(BF16)
        values = legv[s]
        masked = jnp.concatenate([values[16 * i : 16 * i + 16] * mask for i in range(n // 16)], axis=0)
        res[pl.ds(pl.multiple_of(s * pitch, 8), n), :] = lax.dot_general(
            masked, spec[s], NT, preferred_element_type=F32
        )

    def quad(g, carry):
        for copy in loads(g):
            copy.wait()
        for u in range(per):
            one_slot(g * per + u)
        return carry

    def post(src, dst, rsem, ssem, r, dev):
        pltpu.make_async_remote_copy(
            src_ref=src.at[dev], dst_ref=dst.at[r], send_sem=ssem, recv_sem=rsem,
            device_id={"wave": dev}, device_id_type=MESH,
        ).start()

    def post_b(r, dev):
        post(send_b, recv_b, rsem_b, ssem.at[1], r, dev)

    def post_a(r, dev):
        post(send_a, recv_a, rsem_a.at[r // GROUP], ssem.at[0], r, dev)

    def outward(send, high, low):
        def trip(j, carry):
            k = high - j
            for q, chip in ((2 * k - 1, wrapped(z - k, chips)), (2 * k, wrapped(z + k, chips))):
                send(2 * q, 2 * chip + c)
                send(2 * q + 1, 2 * chip + 1 - c)
            return carry

        lax.fori_loop(0, high - low + 1, trip, 0)

    def across(send):
        chip = wrapped(z + chips // 2, chips)
        send(2 * (chips - 1), 2 * chip + c)
        send(2 * (chips - 1) + 1, 2 * chip + 1 - c)

    quad(steps - 1, 0)
    for dev in range(n):
        send_b[dev] = res[pl.ds(HEAD * pitch + dev, tail, stride=pitch), :].astype(BF16)
    recv_b[0] = send_b[w]
    lax.fori_loop(0, steps - 1, quad, 0)
    for dev in range(n):
        send_a[dev] = res[pl.ds(dev, HEAD, stride=pitch), :].astype(BF16)
    recv_a[0] = send_a[w]

    pl.semaphore_wait(barrier, 2 * (2 * near + 1) - 1)
    for chip in (wrapped(z - near, chips), wrapped(z + near, chips)):
        pl.semaphore_signal(far, inc=1, device_id={"wave": 2 * chip + c}, device_id_type=MESH)
    outward(post_a, near, 1)
    outward(post_b, near, 1)
    post_a(1, 2 * z + 1 - c)
    post_b(1, 2 * z + 1 - c)

    def rows_of(r, dev):
        base = dev * slots
        for s in range(HEAD):
            mb[pl.ds(r * HEAD + s, 1), :] = jnp.full((1, LANES), wave[base + s].astype(F32), F32)
        for s in range(tail):
            mb[pl.ds(n * HEAD + r * tail + s, 1), :] = jnp.full(
                (1, LANES), wave[base + HEAD + s].astype(F32), F32
            )

    def place(q, carry):
        d = jnp.where(q % 2 == 1, (q + 1) // 2, -(q // 2))
        chip = wrapped(z + d, chips)
        rows_of(2 * q, 2 * chip + c)
        rows_of(2 * q + 1, 2 * chip + 1 - c)
        return carry

    lax.fori_loop(0, chips, place, 0)

    count = points[0].astype(F32)
    pv = jnp.full((1, LANES), count, F32)
    ip = 1.0 / pv

    def turn(x):
        t = (x - jnp.floor(x * ip + 0.5) * pv) * ip
        u = t * 3.14159265358979
        v = u * u
        sn = u * (1.0 + v * (-1.0 / 6 + v * (1.0 / 120 + v * (-1.0 / 5040 + v * (1.0 / 362880 - v / 39916800)))))
        cs = 1.0 + v * (
            -0.5 + v * (1.0 / 24 + v * (-1.0 / 720 + v * (1.0 / 40320 + v * (-1.0 / 3628800 + v / 479001600))))
        )
        return 1.0 - 2.0 * sn * sn, 2.0 * sn * cs

    span = 32

    def make_basis(i, carry):
        m = mb[pl.ds(pl.multiple_of(i * span, span), span), :]
        pos = lax.broadcasted_iota(jnp.int32, m.shape, 1).astype(F32)
        c0, s0 = turn(m * pos)
        cr, sr = turn(m * float(LANES))
        weight = jnp.where(m == 0.0, 1.0, 2.0)
        weight = jnp.where(2.0 * m < pv, weight, 0.0)
        cv = weight * c0
        sv = -weight * s0
        g = i // (ka // span)
        at = pl.multiple_of((i % (ka // span)) * span, span)
        for j in range(NPAD // LANES):
            cols = slice(j * LANES, (j + 1) * LANES)
            basis[g, pl.ds(at, span), cols] = cv.astype(BF16)
            basis[g, pl.ds(at + ka, span), cols] = sv.astype(BF16)
            cv, sv = cv * cr + sv * sr, sv * cr - cv * sr
        return carry

    trips = mb.shape[0] // span
    lax.fori_loop(groups * (ka // span), trips, make_basis, 0)

    pl.semaphore_wait(far, 2)
    across(post_a)
    across(post_b)
    outward(post_b, chips // 2 - 1, near + 1)
    outward(post_a, chips // 2 - 1, near + 1)

    lax.fori_loop(0, groups * (ka // span), make_basis, 0)

    eye = (
        lax.broadcasted_iota(jnp.int32, (LANES, LANES), 0) == lax.broadcasted_iota(jnp.int32, (LANES, LANES), 1)
    ).astype(F32).astype(BF16)
    first = (lax.broadcasted_iota(jnp.int32, (8, LANES), 1) == 0).astype(F32)
    inv_c = 1.0 / jnp.full((1, ka), cosq[0], F32)

    for g in range(groups + 1):
        qrow[g] = lax.dot_general(
            first, mb[pl.ds(g * ka, ka), :], NT, precision=lax.Precision.HIGHEST, preferred_element_type=F32
        ) / radius

    def derive(g, arrived):
        q = qrow[g, 0:1, :]
        x = lax.dot_general(eye, arrived, NT, preferred_element_type=F32)
        ur, ui, vr, vi, zr, zi, dr, di = (x[half * i : half * (i + 1)] for i in range(8))
        for side, (u, v, ul, vl, zt, dl) in enumerate(
            ((ur, vr, -q * ui, -q * vi, zr, dr), (ui, vi, q * ur, q * vr, zi, di))
        ):
            parts = (u, v, ul, vl, vl * inv_c - zt, dl - ul * inv_c)
            for f, part in enumerate(parts):
                fields[half * f : half * (f + 1), ka * side : ka * (side + 1)] = part.astype(BF16)

    def accumulate(g, opening):
        def column(j, carry):
            at = pl.ds(pl.multiple_of(j * NBLOCK, NBLOCK), NBLOCK)
            new = jnp.dot(fields[...], basis[g, :, at], preferred_element_type=F32)
            acc[:, at] = new if opening else acc[:, at] + new
            return carry

        lax.fori_loop(0, NPAD // NBLOCK, column, 0)

    def quarter(g):
        at = pl.ds(1, GROUP - 1) if g == 0 else pl.ds(g * GROUP, GROUP)
        pltpu.make_async_copy(recv_a.at[at], recv_a.at[at], rsem_a.at[g]).wait()
        derive(g, recv_a[pl.ds(g * GROUP, GROUP)].reshape(ka, LANES))

    last = groups // 2
    for g in range(last):
        quarter(g)
        accumulate(g, g == 0)
    pltpu.make_async_copy(recv_b.at[pl.ds(1, n - 1)], recv_b.at[pl.ds(1, n - 1)], rsem_b).wait()
    derive(groups, recv_b[...].reshape(n * tail, LANES))
    accumulate(groups, False)
    for g in range(groups - 1, last, -1):
        quarter(g)
        accumulate(g, False)
    quarter(last)

    for j in range(NPAD // NBLOCK):
        lo = j * NBLOCK
        hi = min(lo + NBLOCK, NLON)
        new = jnp.dot(fields[...], basis[last, :, lo : lo + NBLOCK], preferred_element_type=F32)
        total = acc[:, lo : lo + NBLOCK] + new
        pos = lax.broadcasted_iota(jnp.int32, total.shape, 1) + lo
        out[0, :, lo:hi] = jnp.where(pos < points[0], total, 0.0).astype(BF16)[:, : hi - lo]

    pltpu.make_async_copy(send_a.at[pl.ds(1, n - 1)], send_a.at[pl.ds(1, n - 1)], ssem.at[0]).wait()
    pltpu.make_async_copy(send_b.at[pl.ds(1, n - 1)], send_b.at[pl.ds(1, n - 1)], ssem.at[1]).wait()


def solution(mesh):
    n = mesh.shape["wave"]

    def body(vort, div, leg, wave, points, cosq):
        slots, rows, nwave = vort.shape
        tail = slots - HEAD
        fields = 12 * rows // 4
        hbm = pl.BlockSpec(memory_space=pltpu.MemorySpace.HBM)
        smem = pl.BlockSpec(memory_space=pltpu.SMEM)
        groups = n // GROUP
        own = -(-slots // 8) * 8
        return pl.pallas_call(
            functools.partial(kernel, n=n, nwave=nwave),
            out_shape=jax.ShapeDtypeStruct((1, fields, NLON), BF16),
            in_specs=[hbm, hbm, hbm, hbm, smem, smem],
            out_specs=pl.BlockSpec(memory_space=pltpu.VMEM),
            scratch_shapes=[
                pltpu.SMEM(wave.shape, wave.dtype),
                pltpu.VMEM((slots, 4 * rows, nwave), BF16),
                pltpu.VMEM((slots, n, nwave), BF16),
                pltpu.VMEM((own, LANES), F32),
                pltpu.VMEM((own, nwave), F32),
                pltpu.VMEM((own, nwave), F32),
                pltpu.VMEM((own, nwave), F32),
                pltpu.VMEM((slots * (n + 8), LANES), F32),
                pltpu.VMEM((n, HEAD, LANES), BF16),
                pltpu.VMEM((n, tail, LANES), BF16),
                pltpu.VMEM((n, HEAD, LANES), BF16),
                pltpu.VMEM((n, tail, LANES), BF16),
                pltpu.VMEM((n * slots, LANES), F32),
                pltpu.VMEM((groups + 1, 2 * GROUP * HEAD, NPAD), BF16),
                pltpu.VMEM((groups + 1, 8, GROUP * HEAD), F32),
                pltpu.VMEM((fields, 2 * GROUP * HEAD), BF16),
                pltpu.VMEM((fields, NPAD), F32),
                pltpu.SemaphoreType.DMA((slots // tail, 3)),
                pltpu.SemaphoreType.DMA,
                pltpu.SemaphoreType.DMA((2,)),
                pltpu.SemaphoreType.DMA((groups,)),
                pltpu.SemaphoreType.DMA,
                pltpu.SemaphoreType.REGULAR,
            ],
            compiler_params=pltpu.CompilerParams(
                collective_id=0, has_side_effects=True, vmem_limit_bytes=46 * 1024 * 1024
            ),
            name="synthesis",
        )(*(pltpu.with_memory_space_constraint(v, pltpu.MemorySpace.HBM) for v in (vort, div, leg, wave)), points, cosq)

    both = P(("member", "wave"), None, None)
    return jax.shard_map(
        body,
        mesh=mesh,
        in_specs=(both, both, P("wave", None, None), P(None), P("wave"), P("wave")),
        out_specs=both,
        check_vma=False,
    )
```

```python
import functools

import jax
import jax.numpy as jnp
from jax import lax
from jax.experimental import pallas as pl
from jax.experimental.pallas import tpu as pltpu
from jax.sharding import PartitionSpec as P

NLON = 5136
MESH = pl.DeviceIdType.MESH
F32 = jnp.float32
BF16 = jnp.bfloat16
LANES = 128
NBLOCK = 768
NPAD = -(-NLON // NBLOCK) * NBLOCK
HEAD = 16
GROUP = 16
NT = (((1,), (1,)), ((), ()))


def wrapped(chip, chips):
    chip = jnp.where(chip >= chips, chip - chips, chip)
    return jnp.where(chip < 0, chip + chips, chip)


def kernel(
    vort, div, leg, wave_in, points, cosq, out,
    wave,
    spec, legv, mown, coef_a, coef_b, coef_c, res,
    send_a, send_b, recv_a, recv_b, mb, basis, qrow, fields, acc,
    in_sem, small_sem, ssem, rsem_a, rsem_b, far,
    *, n, nwave,
):
    w = lax.axis_index("wave")
    z = w // 2
    c = w % 2
    chips = n // 2
    slots = vort.shape[0]
    rows = vort.shape[1]
    half = rows // 2
    tail = slots - HEAD
    radius = nwave / 4.0
    steps = in_sem.shape[0]
    per = slots // steps
    groups = n // GROUP
    ka = GROUP * HEAD

    def loads(g):
        at = pl.ds(g * per, per)
        return (
            pltpu.make_async_copy(vort.at[at], spec.at[at, pl.ds(2 * rows, rows)], in_sem.at[g, 0]),
            pltpu.make_async_copy(div.at[at], spec.at[at, pl.ds(3 * rows, rows)], in_sem.at[g, 1]),
            pltpu.make_async_copy(leg.at[at], legv.at[at], in_sem.at[g, 2]),
        )

    waves = pltpu.make_async_copy(wave_in, wave, small_sem)
    waves.start()
    for g in (steps - 1, *range(steps - 1)):
        for copy in loads(g):
            copy.start()

    barrier = pltpu.get_barrier_semaphore()
    near = chips // 4

    def hello(dev):
        pl.semaphore_signal(barrier, inc=1, device_id={"wave": dev}, device_id_type=MESH)

    def greet(j, carry):
        k = near - j
        for chip in (wrapped(z - k, chips), wrapped(z + k, chips)):
            hello(2 * chip)
            hello(2 * chip + 1)
        return carry

    lax.fori_loop(0, near, greet, 0)
    hello(2 * z + 1 - c)
    waves.wait()

    mown[...] = jnp.zeros_like(mown)
    for s in range(slots):
        mown[s : s + 1, :] = jnp.full((1, LANES), wave[w * slots + s].astype(F32), F32)
    m_own = mown[...]
    lane = lax.broadcasted_iota(jnp.int32, m_own.shape, 1).astype(F32)

    def coupled(deg):
        quotient = jnp.maximum(deg * deg - m_own * m_own, 0.0) / (4.0 * deg * deg - 1.0)
        return -radius * jnp.sqrt(quotient) / deg

    for j in range(nwave // LANES):
        cols = slice(j * LANES, (j + 1) * LANES)
        deg = m_own + (lane + float(j * LANES))
        safe = jnp.maximum(deg, 1.0)
        live = deg < float(nwave)
        coef_a[:, cols] = jnp.where(live & (deg >= 1.0), -radius * m_own / (safe * (safe + 1.0)), 0.0)
        coef_b[:, cols] = jnp.where(deg + 1.0 < float(nwave), coupled(deg + 1.0), 0.0)
        coef_c[:, cols] = jnp.where(live & (deg >= 2.0), coupled(safe), 0.0)

    lane16 = lax.broadcasted_iota(jnp.int32, (16, nwave), 1)
    pitch = n + 8

    def one_slot(s):
        m = wave[w * slots + s]
        a = coef_a[pl.ds(s, 1), :]
        b = coef_b[pl.ds(s, 1), :]
        cc = coef_c[pl.ds(s, 1), :]
        parts = []
        for i in range(4):
            x = spec[s, pl.ds(2 * rows + half * i, half), :].astype(F32)
            up = pltpu.roll(x, nwave - 1, 1)
            down = pltpu.roll(x, 1, 1)
            parts.append((x * a, down * cc - up * b if i < 2 else up * b - down * cc))
        (zr, hzr), (zi, hzi), (dr, hdr), (di, hdi) = parts
        spec[s, pl.ds(0, half), :] = (hzr - di).astype(BF16)
        spec[s, pl.ds(half, half), :] = (dr + hzi).astype(BF16)
        spec[s, pl.ds(2 * half, half), :] = (hdr - zi).astype(BF16)
        spec[s, pl.ds(3 * half, half), :] = (zr + hdi).astype(BF16)
        mask = jnp.where(lane16 < nwave - m, 1.0, 0.0).astype(BF16)
        values = legv[s]
        masked = jnp.concatenate([values[16 * i : 16 * i + 16] * mask for i in range(n // 16)], axis=0)
        res[pl.ds(pl.multiple_of(s * pitch, 8), n), :] = lax.dot_general(
            masked, spec[s], NT, preferred_element_type=F32
        )

    def quad(g, carry):
        for copy in loads(g):
            copy.wait()
        for u in range(per):
            one_slot(g * per + u)
        return carry

    def post(src, dst, rsem, ssem, r, dev):
        pltpu.make_async_remote_copy(
            src_ref=src.at[dev], dst_ref=dst.at[r], send_sem=ssem, recv_sem=rsem,
            device_id={"wave": dev}, device_id_type=MESH,
        ).start()

    def post_b(r, dev):
        post(send_b, recv_b, rsem_b, ssem.at[1], r, dev)

    def post_a(r, dev):
        post(send_a, recv_a, rsem_a.at[r // GROUP], ssem.at[0], r, dev)

    def outward(send, high, low):
        def trip(j, carry):
            k = high - j
            for q, chip in ((2 * k - 1, wrapped(z - k, chips)), (2 * k, wrapped(z + k, chips))):
                send(2 * q, 2 * chip + c)
                send(2 * q + 1, 2 * chip + 1 - c)
            return carry

        lax.fori_loop(0, high - low + 1, trip, 0)

    def across(send):
        chip = wrapped(z + chips // 2, chips)
        send(2 * (chips - 1), 2 * chip + c)
        send(2 * (chips - 1) + 1, 2 * chip + 1 - c)

    quad(steps - 1, 0)
    for dev in range(n):
        send_b[dev] = res[pl.ds(HEAD * pitch + dev, tail, stride=pitch), :].astype(BF16)
    recv_b[0] = send_b[w]
    lax.fori_loop(0, steps - 1, quad, 0)
    for dev in range(n):
        send_a[dev] = res[pl.ds(dev, HEAD, stride=pitch), :].astype(BF16)
    recv_a[0] = send_a[w]

    pl.semaphore_wait(barrier, 2 * (2 * near + 1) - 1)
    for chip in (wrapped(z - near, chips), wrapped(z + near, chips)):
        pl.semaphore_signal(far, inc=1, device_id={"wave": 2 * chip + c}, device_id_type=MESH)
    held = near // 2
    outward(post_a, near, held + 1)
    outward(post_b, near, 1)
    post_a(1, 2 * z + 1 - c)
    post_b(1, 2 * z + 1 - c)

    def rows_of(r, dev):
        base = dev * slots
        for s in range(HEAD):
            mb[pl.ds(r * HEAD + s, 1), :] = jnp.full((1, LANES), wave[base + s].astype(F32), F32)
        for s in range(tail):
            mb[pl.ds(n * HEAD + r * tail + s, 1), :] = jnp.full(
                (1, LANES), wave[base + HEAD + s].astype(F32), F32
            )

    def place(q, carry):
        d = jnp.where(q % 2 == 1, (q + 1) // 2, -(q // 2))
        chip = wrapped(z + d, chips)
        rows_of(2 * q, 2 * chip + c)
        rows_of(2 * q + 1, 2 * chip + 1 - c)
        return carry

    lax.fori_loop(0, chips, place, 0)

    count = points[0].astype(F32)
    pv = jnp.full((1, LANES), count, F32)
    ip = 1.0 / pv

    def turn(x):
        t = (x - jnp.floor(x * ip + 0.5) * pv) * ip
        u = t * 3.14159265358979
        v = u * u
        sn = u * (1.0 + v * (-1.0 / 6 + v * (1.0 / 120 + v * (-1.0 / 5040 + v * (1.0 / 362880 - v / 39916800)))))
        cs = 1.0 + v * (
            -0.5 + v * (1.0 / 24 + v * (-1.0 / 720 + v * (1.0 / 40320 + v * (-1.0 / 3628800 + v / 479001600))))
        )
        return 1.0 - 2.0 * sn * sn, 2.0 * sn * cs

    span = 32

    def make_basis(i, carry):
        m = mb[pl.ds(pl.multiple_of(i * span, span), span), :]
        pos = lax.broadcasted_iota(jnp.int32, m.shape, 1).astype(F32)
        c0, s0 = turn(m * pos)
        cr, sr = turn(m * float(LANES))
        weight = jnp.where(m == 0.0, 1.0, 2.0)
        weight = jnp.where(2.0 * m < pv, weight, 0.0)
        cv = weight * c0
        sv = -weight * s0
        g = i // (ka // span)
        at = pl.multiple_of((i % (ka // span)) * span, span)
        for j in range(NPAD // LANES):
            cols = slice(j * LANES, (j + 1) * LANES)
            basis[g, pl.ds(at, span), cols] = cv.astype(BF16)
            basis[g, pl.ds(at + ka, span), cols] = sv.astype(BF16)
            cv, sv = cv * cr + sv * sr, sv * cr - cv * sr
        return carry

    trips = mb.shape[0] // span
    lax.fori_loop(groups * (ka // span), trips, make_basis, 0)

    pl.semaphore_wait(far, 2)
    across(post_a)
    across(post_b)
    outward(post_b, chips // 2 - 1, near + 1)
    outward(post_a, chips // 2 - 1, near + 1)

    lax.fori_loop(0, groups * (ka // span), make_basis, 0)

    eye = (
        lax.broadcasted_iota(jnp.int32, (LANES, LANES), 0) == lax.broadcasted_iota(jnp.int32, (LANES, LANES), 1)
    ).astype(F32).astype(BF16)
    first = (lax.broadcasted_iota(jnp.int32, (8, LANES), 1) == 0).astype(F32)
    inv_c = 1.0 / jnp.full((1, ka), cosq[0], F32)

    for g in range(groups + 1):
        qrow[g] = lax.dot_general(
            first, mb[pl.ds(g * ka, ka), :], NT, precision=lax.Precision.HIGHEST, preferred_element_type=F32
        ) / radius

    def derive(g, arrived):
        q = qrow[g, 0:1, :]
        x = lax.dot_general(eye, arrived, NT, preferred_element_type=F32)
        ur, ui, vr, vi, zr, zi, dr, di = (x[half * i : half * (i + 1)] for i in range(8))
        for side, (u, v, ul, vl, zt, dl) in enumerate(
            ((ur, vr, -q * ui, -q * vi, zr, dr), (ui, vi, q * ur, q * vr, zi, di))
        ):
            parts = (u, v, ul, vl, vl * inv_c - zt, dl - ul * inv_c)
            for f, part in enumerate(parts):
                fields[half * f : half * (f + 1), ka * side : ka * (side + 1)] = part.astype(BF16)

    def accumulate(g, opening):
        def column(j, carry):
            at = pl.ds(pl.multiple_of(j * NBLOCK, NBLOCK), NBLOCK)
            new = jnp.dot(fields[...], basis[g, :, at], preferred_element_type=F32)
            acc[:, at] = new if opening else acc[:, at] + new
            return carry

        lax.fori_loop(0, NPAD // NBLOCK, column, 0)

    def quarter(g):
        at = pl.ds(1, GROUP - 1) if g == 0 else pl.ds(g * GROUP, GROUP)
        pltpu.make_async_copy(recv_a.at[at], recv_a.at[at], rsem_a.at[g]).wait()
        derive(g, recv_a[pl.ds(g * GROUP, GROUP)].reshape(ka, LANES))

    last = groups // 2
    pltpu.make_async_copy(recv_b.at[pl.ds(1, n - 1)], recv_b.at[pl.ds(1, n - 1)], rsem_b).wait()
    outward(post_a, held, 1)
    derive(groups, recv_b[...].reshape(n * tail, LANES))
    accumulate(groups, True)
    for g in (*range(last - 1, -1, -1), *range(groups - 1, last, -1)):
        quarter(g)
        accumulate(g, False)
    quarter(last)

    for j in range(NPAD // NBLOCK):
        lo = j * NBLOCK
        hi = min(lo + NBLOCK, NLON)
        new = jnp.dot(fields[...], basis[last, :, lo : lo + NBLOCK], preferred_element_type=F32)
        total = acc[:, lo : lo + NBLOCK] + new
        pos = lax.broadcasted_iota(jnp.int32, total.shape, 1) + lo
        out[0, :, lo:hi] = jnp.where(pos < points[0], total, 0.0).astype(BF16)[:, : hi - lo]

    pltpu.make_async_copy(send_a.at[pl.ds(1, n - 1)], send_a.at[pl.ds(1, n - 1)], ssem.at[0]).wait()
    pltpu.make_async_copy(send_b.at[pl.ds(1, n - 1)], send_b.at[pl.ds(1, n - 1)], ssem.at[1]).wait()


def solution(mesh):
    n = mesh.shape["wave"]

    def body(vort, div, leg, wave, points, cosq):
        slots, rows, nwave = vort.shape
        tail = slots - HEAD
        fields = 12 * rows // 4
        hbm = pl.BlockSpec(memory_space=pltpu.MemorySpace.HBM)
        smem = pl.BlockSpec(memory_space=pltpu.SMEM)
        groups = n // GROUP
        own = -(-slots // 8) * 8
        return pl.pallas_call(
            functools.partial(kernel, n=n, nwave=nwave),
            out_shape=jax.ShapeDtypeStruct((1, fields, NLON), BF16),
            in_specs=[hbm, hbm, hbm, hbm, smem, smem],
            out_specs=pl.BlockSpec(memory_space=pltpu.VMEM),
            scratch_shapes=[
                pltpu.SMEM(wave.shape, wave.dtype),
                pltpu.VMEM((slots, 4 * rows, nwave), BF16),
                pltpu.VMEM((slots, n, nwave), BF16),
                pltpu.VMEM((own, LANES), F32),
                pltpu.VMEM((own, nwave), F32),
                pltpu.VMEM((own, nwave), F32),
                pltpu.VMEM((own, nwave), F32),
                pltpu.VMEM((slots * (n + 8), LANES), F32),
                pltpu.VMEM((n, HEAD, LANES), BF16),
                pltpu.VMEM((n, tail, LANES), BF16),
                pltpu.VMEM((n, HEAD, LANES), BF16),
                pltpu.VMEM((n, tail, LANES), BF16),
                pltpu.VMEM((n * slots, LANES), F32),
                pltpu.VMEM((groups + 1, 2 * GROUP * HEAD, NPAD), BF16),
                pltpu.VMEM((groups + 1, 8, GROUP * HEAD), F32),
                pltpu.VMEM((fields, 2 * GROUP * HEAD), BF16),
                pltpu.VMEM((fields, NPAD), F32),
                pltpu.SemaphoreType.DMA((slots // tail, 3)),
                pltpu.SemaphoreType.DMA,
                pltpu.SemaphoreType.DMA((2,)),
                pltpu.SemaphoreType.DMA((groups,)),
                pltpu.SemaphoreType.DMA,
                pltpu.SemaphoreType.REGULAR,
            ],
            compiler_params=pltpu.CompilerParams(
                collective_id=0, has_side_effects=True, vmem_limit_bytes=46 * 1024 * 1024
            ),
            name="synthesis",
        )(*(pltpu.with_memory_space_constraint(v, pltpu.MemorySpace.HBM) for v in (vort, div, leg, wave)), points, cosq)

    both = P(("member", "wave"), None, None)
    return jax.shard_map(
        body,
        mesh=mesh,
        in_specs=(both, both, P("wave", None, None), P(None), P("wave"), P("wave")),
        out_specs=both,
        check_vma=False,
    )
```

```python
import functools

import jax
import jax.numpy as jnp
from jax import lax
from jax.experimental import pallas as pl
from jax.experimental.pallas import tpu as pltpu
from jax.sharding import PartitionSpec as P

NLON = 5136
MESH = pl.DeviceIdType.MESH
F32 = jnp.float32
BF16 = jnp.bfloat16
LANES = 128
NBLOCK = 768
NPAD = -(-NLON // NBLOCK) * NBLOCK
HEAD = 16
GROUP = 16
NT = (((1,), (1,)), ((), ()))


def wrapped(chip, chips):
    chip = jnp.where(chip >= chips, chip - chips, chip)
    return jnp.where(chip < 0, chip + chips, chip)


def kernel(
    vort, div, leg, wave_in, points, cosq, out,
    wave,
    spec, legv, mown, coef_a, coef_b, coef_c, res,
    send_a, send_b, recv_a, recv_b, mb, basis, qrow, fields, acc,
    in_sem, small_sem, ssem, rsem_a, rsem_b, far,
    *, n, nwave,
):
    w = lax.axis_index("wave")
    z = w // 2
    c = w % 2
    chips = n // 2
    slots = vort.shape[0]
    rows = vort.shape[1]
    half = rows // 2
    tail = slots - HEAD
    radius = nwave / 4.0
    steps = in_sem.shape[0]
    per = slots // steps
    groups = n // GROUP
    ka = GROUP * HEAD

    def loads(g):
        at = pl.ds(g * per, per)
        return (
            pltpu.make_async_copy(vort.at[at], spec.at[at, pl.ds(2 * rows, rows)], in_sem.at[g, 0]),
            pltpu.make_async_copy(div.at[at], spec.at[at, pl.ds(3 * rows, rows)], in_sem.at[g, 1]),
            pltpu.make_async_copy(leg.at[at], legv.at[at], in_sem.at[g, 2]),
        )

    waves = pltpu.make_async_copy(wave_in, wave, small_sem)
    waves.start()
    for g in (steps - 1, *range(steps - 1)):
        for copy in loads(g):
            copy.start()

    barrier = pltpu.get_barrier_semaphore()
    near = chips // 4

    def hello(dev):
        pl.semaphore_signal(barrier, inc=1, device_id={"wave": dev}, device_id_type=MESH)

    def greet(j, carry):
        k = near - j
        for chip in (wrapped(z - k, chips), wrapped(z + k, chips)):
            hello(2 * chip)
            hello(2 * chip + 1)
        return carry

    lax.fori_loop(0, near, greet, 0)
    hello(2 * z + 1 - c)
    waves.wait()

    mown[...] = jnp.zeros_like(mown)
    for s in range(slots):
        mown[s : s + 1, :] = jnp.full((1, LANES), wave[w * slots + s].astype(F32), F32)
    m_own = mown[...]
    lane = lax.broadcasted_iota(jnp.int32, m_own.shape, 1).astype(F32)

    def coupled(deg):
        quotient = jnp.maximum(deg * deg - m_own * m_own, 0.0) / (4.0 * deg * deg - 1.0)
        return -radius * jnp.sqrt(quotient) / deg

    for j in range(nwave // LANES):
        cols = slice(j * LANES, (j + 1) * LANES)
        deg = m_own + (lane + float(j * LANES))
        safe = jnp.maximum(deg, 1.0)
        live = deg < float(nwave)
        coef_a[:, cols] = jnp.where(live & (deg >= 1.0), -radius * m_own / (safe * (safe + 1.0)), 0.0)
        coef_b[:, cols] = jnp.where(deg + 1.0 < float(nwave), coupled(deg + 1.0), 0.0)
        coef_c[:, cols] = jnp.where(live & (deg >= 2.0), coupled(safe), 0.0)

    lane16 = lax.broadcasted_iota(jnp.int32, (16, nwave), 1)
    pitch = n + 8

    def one_slot(s):
        m = wave[w * slots + s]
        a = coef_a[pl.ds(s, 1), :]
        b = coef_b[pl.ds(s, 1), :]
        cc = coef_c[pl.ds(s, 1), :]
        parts = []
        for i in range(4):
            x = spec[s, pl.ds(2 * rows + half * i, half), :].astype(F32)
            up = pltpu.roll(x, nwave - 1, 1)
            down = pltpu.roll(x, 1, 1)
            parts.append((x * a, down * cc - up * b if i < 2 else up * b - down * cc))
        (zr, hzr), (zi, hzi), (dr, hdr), (di, hdi) = parts
        spec[s, pl.ds(0, half), :] = (hzr - di).astype(BF16)
        spec[s, pl.ds(half, half), :] = (dr + hzi).astype(BF16)
        spec[s, pl.ds(2 * half, half), :] = (hdr - zi).astype(BF16)
        spec[s, pl.ds(3 * half, half), :] = (zr + hdi).astype(BF16)
        mask = jnp.where(lane16 < nwave - m, 1.0, 0.0).astype(BF16)
        values = legv[s]
        masked = jnp.concatenate([values[16 * i : 16 * i + 16] * mask for i in range(n // 16)], axis=0)
        res[pl.ds(pl.multiple_of(s * pitch, 8), n), :] = lax.dot_general(
            masked, spec[s], NT, preferred_element_type=F32
        )

    def quad(g, carry):
        for copy in loads(g):
            copy.wait()
        for u in range(per):
            one_slot(g * per + u)
        return carry

    def post(src, dst, rsem, ssem, r, dev):
        pltpu.make_async_remote_copy(
            src_ref=src.at[dev], dst_ref=dst.at[r], send_sem=ssem, recv_sem=rsem,
            device_id={"wave": dev}, device_id_type=MESH,
        ).start()

    def post_b(r, dev):
        post(send_b, recv_b, rsem_b, ssem.at[1], r, dev)

    def post_a(r, dev):
        post(send_a, recv_a, rsem_a.at[r // GROUP], ssem.at[0], r, dev)

    def outward(send, high, low):
        def trip(j, carry):
            k = high - j
            for q, chip in ((2 * k - 1, wrapped(z - k, chips)), (2 * k, wrapped(z + k, chips))):
                send(2 * q, 2 * chip + c)
                send(2 * q + 1, 2 * chip + 1 - c)
            return carry

        lax.fori_loop(0, high - low + 1, trip, 0)

    def across(send):
        chip = wrapped(z + chips // 2, chips)
        send(2 * (chips - 1), 2 * chip + c)
        send(2 * (chips - 1) + 1, 2 * chip + 1 - c)

    quad(steps - 1, 0)
    for dev in range(n):
        send_b[dev] = res[pl.ds(HEAD * pitch + dev, tail, stride=pitch), :].astype(BF16)
    recv_b[0] = send_b[w]
    lax.fori_loop(0, steps - 1, quad, 0)
    for dev in range(n):
        send_a[dev] = res[pl.ds(dev, HEAD, stride=pitch), :].astype(BF16)
    recv_a[0] = send_a[w]

    pl.semaphore_wait(barrier, 2 * (2 * near + 1) - 1)
    for chip in (wrapped(z - near, chips), wrapped(z + near, chips)):
        pl.semaphore_signal(far, inc=1, device_id={"wave": 2 * chip + c}, device_id_type=MESH)
    held = near // 2 - 1
    outward(post_a, near, held + 1)
    outward(post_b, near, 1)
    post_a(1, 2 * z + 1 - c)
    post_b(1, 2 * z + 1 - c)

    def rows_of(r, dev):
        base = dev * slots
        for s in range(HEAD):
            mb[pl.ds(r * HEAD + s, 1), :] = jnp.full((1, LANES), wave[base + s].astype(F32), F32)
        for s in range(tail):
            mb[pl.ds(n * HEAD + r * tail + s, 1), :] = jnp.full(
                (1, LANES), wave[base + HEAD + s].astype(F32), F32
            )

    def place(q, carry):
        d = jnp.where(q % 2 == 1, (q + 1) // 2, -(q // 2))
        chip = wrapped(z + d, chips)
        rows_of(2 * q, 2 * chip + c)
        rows_of(2 * q + 1, 2 * chip + 1 - c)
        return carry

    lax.fori_loop(0, chips, place, 0)

    count = points[0].astype(F32)
    pv = jnp.full((1, LANES), count, F32)
    ip = 1.0 / pv

    def turn(x):
        t = (x - jnp.floor(x * ip + 0.5) * pv) * ip
        u = t * 3.14159265358979
        v = u * u
        sn = u * (1.0 + v * (-1.0 / 6 + v * (1.0 / 120 + v * (-1.0 / 5040 + v * (1.0 / 362880 - v / 39916800)))))
        cs = 1.0 + v * (
            -0.5 + v * (1.0 / 24 + v * (-1.0 / 720 + v * (1.0 / 40320 + v * (-1.0 / 3628800 + v / 479001600))))
        )
        return 1.0 - 2.0 * sn * sn, 2.0 * sn * cs

    span = 32

    def make_basis(i, carry):
        m = mb[pl.ds(pl.multiple_of(i * span, span), span), :]
        pos = lax.broadcasted_iota(jnp.int32, m.shape, 1).astype(F32)
        c0, s0 = turn(m * pos)
        cr, sr = turn(m * float(LANES))
        weight = jnp.where(m == 0.0, 1.0, 2.0)
        weight = jnp.where(2.0 * m < pv, weight, 0.0)
        cv = weight * c0
        sv = -weight * s0
        g = i // (ka // span)
        at = pl.multiple_of((i % (ka // span)) * span, span)
        for j in range(NPAD // LANES):
            cols = slice(j * LANES, (j + 1) * LANES)
            basis[g, pl.ds(at, span), cols] = cv.astype(BF16)
            basis[g, pl.ds(at + ka, span), cols] = sv.astype(BF16)
            cv, sv = cv * cr + sv * sr, sv * cr - cv * sr
        return carry

    trips = mb.shape[0] // span
    lax.fori_loop(groups * (ka // span), trips, make_basis, 0)

    pl.semaphore_wait(far, 2)
    across(post_a)
    across(post_b)
    outward(post_b, chips // 2 - 1, near + 1)
    outward(post_a, chips // 2 - 1, near + 1)
    outward(post_a, held, 1)

    lax.fori_loop(0, groups * (ka // span), make_basis, 0)

    eye = (
        lax.broadcasted_iota(jnp.int32, (LANES, LANES), 0) == lax.broadcasted_iota(jnp.int32, (LANES, LANES), 1)
    ).astype(F32).astype(BF16)
    first = (lax.broadcasted_iota(jnp.int32, (8, LANES), 1) == 0).astype(F32)
    inv_c = 1.0 / jnp.full((1, ka), cosq[0], F32)

    for g in range(groups + 1):
        qrow[g] = lax.dot_general(
            first, mb[pl.ds(g * ka, ka), :], NT, precision=lax.Precision.HIGHEST, preferred_element_type=F32
        ) / radius

    def derive(g, arrived):
        q = qrow[g, 0:1, :]
        x = lax.dot_general(eye, arrived, NT, preferred_element_type=F32)
        ur, ui, vr, vi, zr, zi, dr, di = (x[half * i : half * (i + 1)] for i in range(8))
        for side, (u, v, ul, vl, zt, dl) in enumerate(
            ((ur, vr, -q * ui, -q * vi, zr, dr), (ui, vi, q * ur, q * vr, zi, di))
        ):
            parts = (u, v, ul, vl, vl * inv_c - zt, dl - ul * inv_c)
            for f, part in enumerate(parts):
                fields[half * f : half * (f + 1), ka * side : ka * (side + 1)] = part.astype(BF16)

    def accumulate(g, opening):
        def column(j, carry):
            at = pl.ds(pl.multiple_of(j * NBLOCK, NBLOCK), NBLOCK)
            new = jnp.dot(fields[...], basis[g, :, at], preferred_element_type=F32)
            acc[:, at] = new if opening else acc[:, at] + new
            return carry

        lax.fori_loop(0, NPAD // NBLOCK, column, 0)

    def quarter(g):
        at = pl.ds(1, GROUP - 1) if g == 0 else pl.ds(g * GROUP, GROUP)
        pltpu.make_async_copy(recv_a.at[at], recv_a.at[at], rsem_a.at[g]).wait()
        derive(g, recv_a[pl.ds(g * GROUP, GROUP)].reshape(ka, LANES))

    last = 0
    quarter(1)
    accumulate(1, True)
    pltpu.make_async_copy(recv_b.at[pl.ds(1, n - 1)], recv_b.at[pl.ds(1, n - 1)], rsem_b).wait()
    derive(groups, recv_b[...].reshape(n * tail, LANES))
    accumulate(groups, False)
    for g in range(groups - 1, 1, -1):
        quarter(g)
        accumulate(g, False)
    quarter(last)

    for j in range(NPAD // NBLOCK):
        lo = j * NBLOCK
        hi = min(lo + NBLOCK, NLON)
        new = jnp.dot(fields[...], basis[last, :, lo : lo + NBLOCK], preferred_element_type=F32)
        total = acc[:, lo : lo + NBLOCK] + new
        pos = lax.broadcasted_iota(jnp.int32, total.shape, 1) + lo
        out[0, :, lo:hi] = jnp.where(pos < points[0], total, 0.0).astype(BF16)[:, : hi - lo]

    pltpu.make_async_copy(send_a.at[pl.ds(1, n - 1)], send_a.at[pl.ds(1, n - 1)], ssem.at[0]).wait()
    pltpu.make_async_copy(send_b.at[pl.ds(1, n - 1)], send_b.at[pl.ds(1, n - 1)], ssem.at[1]).wait()


def solution(mesh):
    n = mesh.shape["wave"]

    def body(vort, div, leg, wave, points, cosq):
        slots, rows, nwave = vort.shape
        tail = slots - HEAD
        fields = 12 * rows // 4
        hbm = pl.BlockSpec(memory_space=pltpu.MemorySpace.HBM)
        smem = pl.BlockSpec(memory_space=pltpu.SMEM)
        groups = n // GROUP
        own = -(-slots // 8) * 8
        return pl.pallas_call(
            functools.partial(kernel, n=n, nwave=nwave),
            out_shape=jax.ShapeDtypeStruct((1, fields, NLON), BF16),
            in_specs=[hbm, hbm, hbm, hbm, smem, smem],
            out_specs=pl.BlockSpec(memory_space=pltpu.VMEM),
            scratch_shapes=[
                pltpu.SMEM(wave.shape, wave.dtype),
                pltpu.VMEM((slots, 4 * rows, nwave), BF16),
                pltpu.VMEM((slots, n, nwave), BF16),
                pltpu.VMEM((own, LANES), F32),
                pltpu.VMEM((own, nwave), F32),
                pltpu.VMEM((own, nwave), F32),
                pltpu.VMEM((own, nwave), F32),
                pltpu.VMEM((slots * (n + 8), LANES), F32),
                pltpu.VMEM((n, HEAD, LANES), BF16),
                pltpu.VMEM((n, tail, LANES), BF16),
                pltpu.VMEM((n, HEAD, LANES), BF16),
                pltpu.VMEM((n, tail, LANES), BF16),
                pltpu.VMEM((n * slots, LANES), F32),
                pltpu.VMEM((groups + 1, 2 * GROUP * HEAD, NPAD), BF16),
                pltpu.VMEM((groups + 1, 8, GROUP * HEAD), F32),
                pltpu.VMEM((fields, 2 * GROUP * HEAD), BF16),
                pltpu.VMEM((fields, NPAD), F32),
                pltpu.SemaphoreType.DMA((slots // tail, 3)),
                pltpu.SemaphoreType.DMA,
                pltpu.SemaphoreType.DMA((2,)),
                pltpu.SemaphoreType.DMA((groups,)),
                pltpu.SemaphoreType.DMA,
                pltpu.SemaphoreType.REGULAR,
            ],
            compiler_params=pltpu.CompilerParams(
                collective_id=0, has_side_effects=True, vmem_limit_bytes=46 * 1024 * 1024
            ),
            name="synthesis",
        )(*(pltpu.with_memory_space_constraint(v, pltpu.MemorySpace.HBM) for v in (vort, div, leg, wave)), points, cosq)

    both = P(("member", "wave"), None, None)
    return jax.shard_map(
        body,
        mesh=mesh,
        in_specs=(both, both, P("wave", None, None), P(None), P("wave"), P("wave")),
        out_specs=both,
        check_vma=False,
    )
```

```python
import functools

import jax
import jax.numpy as jnp
from jax import lax
from jax.experimental import pallas as pl
from jax.experimental.pallas import tpu as pltpu
from jax.sharding import PartitionSpec as P

NLON = 5136
MESH = pl.DeviceIdType.MESH
F32 = jnp.float32
BF16 = jnp.bfloat16
LANES = 128
NBLOCK = 768
NPAD = -(-NLON // NBLOCK) * NBLOCK
HEAD = 16
GROUP = 16
NT = (((1,), (1,)), ((), ()))


def wrapped(chip, chips):
    chip = jnp.where(chip >= chips, chip - chips, chip)
    return jnp.where(chip < 0, chip + chips, chip)


def kernel(
    vort, div, leg, wave_in, points, cosq, out,
    wave,
    spec, legv, mown, coef_a, coef_b, coef_c, res,
    send_a, send_b, recv_a, recv_b, mb, basis, qrow, fields, acc,
    in_sem, small_sem, ssem, rsem_a, rsem_b, far,
    *, n, nwave,
):
    w = lax.axis_index("wave")
    z = w // 2
    c = w % 2
    chips = n // 2
    slots = vort.shape[0]
    rows = vort.shape[1]
    half = rows // 2
    tail = slots - HEAD
    radius = nwave / 4.0
    steps = in_sem.shape[0]
    per = slots // steps
    groups = n // GROUP
    ka = GROUP * HEAD

    def loads(g):
        at = pl.ds(g * per, per)
        return (
            pltpu.make_async_copy(vort.at[at], spec.at[at, pl.ds(2 * rows, rows)], in_sem.at[g, 0]),
            pltpu.make_async_copy(div.at[at], spec.at[at, pl.ds(3 * rows, rows)], in_sem.at[g, 1]),
            pltpu.make_async_copy(leg.at[at], legv.at[at], in_sem.at[g, 2]),
        )

    waves = pltpu.make_async_copy(wave_in, wave, small_sem)
    waves.start()
    for copy in loads(steps - 1):
        copy.start()

    barrier = pltpu.get_barrier_semaphore()
    near = chips // 4

    def hello(dev):
        pl.semaphore_signal(barrier, inc=1, device_id={"wave": dev}, device_id_type=MESH)

    def greet(j, carry):
        k = near - j
        for chip in (wrapped(z - k, chips), wrapped(z + k, chips)):
            hello(2 * chip)
            hello(2 * chip + 1)
        return carry

    greet(0, 0)
    for g in range(steps - 1):
        for copy in loads(g):
            copy.start()
    lax.fori_loop(1, near, greet, 0)
    hello(2 * z + 1 - c)
    waves.wait()

    mown[...] = jnp.zeros_like(mown)
    for s in range(slots):
        mown[s : s + 1, :] = jnp.full((1, LANES), wave[w * slots + s].astype(F32), F32)
    m_own = mown[...]
    lane = lax.broadcasted_iota(jnp.int32, m_own.shape, 1).astype(F32)

    def coupled(deg):
        quotient = jnp.maximum(deg * deg - m_own * m_own, 0.0) / (4.0 * deg * deg - 1.0)
        return -radius * jnp.sqrt(quotient) / deg

    for j in range(nwave // LANES):
        cols = slice(j * LANES, (j + 1) * LANES)
        deg = m_own + (lane + float(j * LANES))
        safe = jnp.maximum(deg, 1.0)
        live = deg < float(nwave)
        coef_a[:, cols] = jnp.where(live & (deg >= 1.0), -radius * m_own / (safe * (safe + 1.0)), 0.0)
        coef_b[:, cols] = jnp.where(deg + 1.0 < float(nwave), coupled(deg + 1.0), 0.0)
        coef_c[:, cols] = jnp.where(live & (deg >= 2.0), coupled(safe), 0.0)

    lane16 = lax.broadcasted_iota(jnp.int32, (16, nwave), 1)
    pitch = n + 8

    def one_slot(s):
        m = wave[w * slots + s]
        a = coef_a[pl.ds(s, 1), :]
        b = coef_b[pl.ds(s, 1), :]
        cc = coef_c[pl.ds(s, 1), :]
        parts = []
        for i in range(4):
            x = spec[s, pl.ds(2 * rows + half * i, half), :].astype(F32)
            up = pltpu.roll(x, nwave - 1, 1)
            down = pltpu.roll(x, 1, 1)
            parts.append((x * a, down * cc - up * b if i < 2 else up * b - down * cc))
        (zr, hzr), (zi, hzi), (dr, hdr), (di, hdi) = parts
        spec[s, pl.ds(0, half), :] = (hzr - di).astype(BF16)
        spec[s, pl.ds(half, half), :] = (dr + hzi).astype(BF16)
        spec[s, pl.ds(2 * half, half), :] = (hdr - zi).astype(BF16)
        spec[s, pl.ds(3 * half, half), :] = (zr + hdi).astype(BF16)
        mask = jnp.where(lane16 < nwave - m, 1.0, 0.0).astype(BF16)
        values = legv[s]
        masked = jnp.concatenate([values[16 * i : 16 * i + 16] * mask for i in range(n // 16)], axis=0)
        res[pl.ds(pl.multiple_of(s * pitch, 8), n), :] = lax.dot_general(
            masked, spec[s], NT, preferred_element_type=F32
        )

    def quad(g, carry):
        for copy in loads(g):
            copy.wait()
        for u in range(per):
            one_slot(g * per + u)
        return carry

    def post(src, dst, rsem, ssem, r, dev):
        pltpu.make_async_remote_copy(
            src_ref=src.at[dev], dst_ref=dst.at[r], send_sem=ssem, recv_sem=rsem,
            device_id={"wave": dev}, device_id_type=MESH,
        ).start()

    def post_b(r, dev):
        post(send_b, recv_b, rsem_b, ssem.at[1], r, dev)

    def post_a(r, dev):
        post(send_a, recv_a, rsem_a.at[r // GROUP], ssem.at[0], r, dev)

    def outward(send, high, low):
        def trip(j, carry):
            k = high - j
            for q, chip in ((2 * k - 1, wrapped(z - k, chips)), (2 * k, wrapped(z + k, chips))):
                send(2 * q, 2 * chip + c)
                send(2 * q + 1, 2 * chip + 1 - c)
            return carry

        lax.fori_loop(0, high - low + 1, trip, 0)

    def across(send):
        chip = wrapped(z + chips // 2, chips)
        send(2 * (chips - 1), 2 * chip + c)
        send(2 * (chips - 1) + 1, 2 * chip + 1 - c)

    quad(steps - 1, 0)
    for dev in range(n):
        send_b[dev] = res[pl.ds(HEAD * pitch + dev, tail, stride=pitch), :].astype(BF16)
    recv_b[0] = send_b[w]
    lax.fori_loop(0, steps - 1, quad, 0)
    for dev in range(n):
        send_a[dev] = res[pl.ds(dev, HEAD, stride=pitch), :].astype(BF16)
    recv_a[0] = send_a[w]

    pl.semaphore_wait(barrier, 2 * (2 * near + 1) - 1)
    for chip in (wrapped(z - near, chips), wrapped(z + near, chips)):
        pl.semaphore_signal(far, inc=1, device_id={"wave": 2 * chip + c}, device_id_type=MESH)
    outward(post_a, near, 1)
    outward(post_b, near, 1)
    post_a(1, 2 * z + 1 - c)
    post_b(1, 2 * z + 1 - c)

    def rows_of(r, dev):
        base = dev * slots
        for s in range(HEAD):
            mb[pl.ds(r * HEAD + s, 1), :] = jnp.full((1, LANES), wave[base + s].astype(F32), F32)
        for s in range(tail):
            mb[pl.ds(n * HEAD + r * tail + s, 1), :] = jnp.full(
                (1, LANES), wave[base + HEAD + s].astype(F32), F32
            )

    def place(q, carry):
        d = jnp.where(q % 2 == 1, (q + 1) // 2, -(q // 2))
        chip = wrapped(z + d, chips)
        rows_of(2 * q, 2 * chip + c)
        rows_of(2 * q + 1, 2 * chip + 1 - c)
        return carry

    lax.fori_loop(0, chips, place, 0)

    count = points[0].astype(F32)
    pv = jnp.full((1, LANES), count, F32)
    ip = 1.0 / pv

    def turn(x):
        t = (x - jnp.floor(x * ip + 0.5) * pv) * ip
        u = t * 3.14159265358979
        v = u * u
        sn = u * (1.0 + v * (-1.0 / 6 + v * (1.0 / 120 + v * (-1.0 / 5040 + v * (1.0 / 362880 - v / 39916800)))))
        cs = 1.0 + v * (
            -0.5 + v * (1.0 / 24 + v * (-1.0 / 720 + v * (1.0 / 40320 + v * (-1.0 / 3628800 + v / 479001600))))
        )
        return 1.0 - 2.0 * sn * sn, 2.0 * sn * cs

    span = 32

    def make_basis(i, carry):
        m = mb[pl.ds(pl.multiple_of(i * span, span), span), :]
        pos = lax.broadcasted_iota(jnp.int32, m.shape, 1).astype(F32)
        c0, s0 = turn(m * pos)
        cr, sr = turn(m * float(LANES))
        weight = jnp.where(m == 0.0, 1.0, 2.0)
        weight = jnp.where(2.0 * m < pv, weight, 0.0)
        cv = weight * c0
        sv = -weight * s0
        g = i // (ka // span)
        at = pl.multiple_of((i % (ka // span)) * span, span)
        for j in range(NPAD // LANES):
            cols = slice(j * LANES, (j + 1) * LANES)
            basis[g, pl.ds(at, span), cols] = cv.astype(BF16)
            basis[g, pl.ds(at + ka, span), cols] = sv.astype(BF16)
            cv, sv = cv * cr + sv * sr, sv * cr - cv * sr
        return carry

    trips = mb.shape[0] // span
    lax.fori_loop(groups * (ka // span), trips, make_basis, 0)

    pl.semaphore_wait(far, 2)
    across(post_a)
    across(post_b)
    outward(post_b, chips // 2 - 1, near + 1)
    outward(post_a, chips // 2 - 1, near + 1)

    lax.fori_loop(0, groups * (ka // span), make_basis, 0)

    eye = (
        lax.broadcasted_iota(jnp.int32, (LANES, LANES), 0) == lax.broadcasted_iota(jnp.int32, (LANES, LANES), 1)
    ).astype(F32).astype(BF16)
    first = (lax.broadcasted_iota(jnp.int32, (8, LANES), 1) == 0).astype(F32)
    inv_c = 1.0 / jnp.full((1, ka), cosq[0], F32)

    for g in range(groups + 1):
        qrow[g] = lax.dot_general(
            first, mb[pl.ds(g * ka, ka), :], NT, precision=lax.Precision.HIGHEST, preferred_element_type=F32
        ) / radius

    def derive(g, arrived):
        q = qrow[g, 0:1, :]
        x = lax.dot_general(eye, arrived, NT, preferred_element_type=F32)
        ur, ui, vr, vi, zr, zi, dr, di = (x[half * i : half * (i + 1)] for i in range(8))
        for side, (u, v, ul, vl, zt, dl) in enumerate(
            ((ur, vr, -q * ui, -q * vi, zr, dr), (ui, vi, q * ur, q * vr, zi, di))
        ):
            parts = (u, v, ul, vl, vl * inv_c - zt, dl - ul * inv_c)
            for f, part in enumerate(parts):
                fields[half * f : half * (f + 1), ka * side : ka * (side + 1)] = part.astype(BF16)

    def accumulate(g, opening):
        def column(j, carry):
            at = pl.ds(pl.multiple_of(j * NBLOCK, NBLOCK), NBLOCK)
            new = jnp.dot(fields[...], basis[g, :, at], preferred_element_type=F32)
            acc[:, at] = new if opening else acc[:, at] + new
            return carry

        lax.fori_loop(0, NPAD // NBLOCK, column, 0)

    def quarter(g):
        at = pl.ds(1, GROUP - 1) if g == 0 else pl.ds(g * GROUP, GROUP)
        pltpu.make_async_copy(recv_a.at[at], recv_a.at[at], rsem_a.at[g]).wait()
        derive(g, recv_a[pl.ds(g * GROUP, GROUP)].reshape(ka, LANES))

    last = groups // 2
    for g in range(last):
        quarter(g)
        accumulate(g, g == 0)
    pltpu.make_async_copy(recv_b.at[pl.ds(1, n - 1)], recv_b.at[pl.ds(1, n - 1)], rsem_b).wait()
    derive(groups, recv_b[...].reshape(n * tail, LANES))
    accumulate(groups, False)
    for g in range(groups - 1, last, -1):
        quarter(g)
        accumulate(g, False)
    quarter(last)

    for j in range(NPAD // NBLOCK):
        lo = j * NBLOCK
        hi = min(lo + NBLOCK, NLON)
        new = jnp.dot(fields[...], basis[last, :, lo : lo + NBLOCK], preferred_element_type=F32)
        total = acc[:, lo : lo + NBLOCK] + new
        pos = lax.broadcasted_iota(jnp.int32, total.shape, 1) + lo
        out[0, :, lo:hi] = jnp.where(pos < points[0], total, 0.0).astype(BF16)[:, : hi - lo]

    pltpu.make_async_copy(send_a.at[pl.ds(1, n - 1)], send_a.at[pl.ds(1, n - 1)], ssem.at[0]).wait()
    pltpu.make_async_copy(send_b.at[pl.ds(1, n - 1)], send_b.at[pl.ds(1, n - 1)], ssem.at[1]).wait()


def solution(mesh):
    n = mesh.shape["wave"]

    def body(vort, div, leg, wave, points, cosq):
        slots, rows, nwave = vort.shape
        tail = slots - HEAD
        fields = 12 * rows // 4
        hbm = pl.BlockSpec(memory_space=pltpu.MemorySpace.HBM)
        smem = pl.BlockSpec(memory_space=pltpu.SMEM)
        groups = n // GROUP
        own = -(-slots // 8) * 8
        return pl.pallas_call(
            functools.partial(kernel, n=n, nwave=nwave),
            out_shape=jax.ShapeDtypeStruct((1, fields, NLON), BF16),
            in_specs=[hbm, hbm, hbm, hbm, smem, smem],
            out_specs=pl.BlockSpec(memory_space=pltpu.VMEM),
            scratch_shapes=[
                pltpu.SMEM(wave.shape, wave.dtype),
                pltpu.VMEM((slots, 4 * rows, nwave), BF16),
                pltpu.VMEM((slots, n, nwave), BF16),
                pltpu.VMEM((own, LANES), F32),
                pltpu.VMEM((own, nwave), F32),
                pltpu.VMEM((own, nwave), F32),
                pltpu.VMEM((own, nwave), F32),
                pltpu.VMEM((slots * (n + 8), LANES), F32),
                pltpu.VMEM((n, HEAD, LANES), BF16),
                pltpu.VMEM((n, tail, LANES), BF16),
                pltpu.VMEM((n, HEAD, LANES), BF16),
                pltpu.VMEM((n, tail, LANES), BF16),
                pltpu.VMEM((n * slots, LANES), F32),
                pltpu.VMEM((groups + 1, 2 * GROUP * HEAD, NPAD), BF16),
                pltpu.VMEM((groups + 1, 8, GROUP * HEAD), F32),
                pltpu.VMEM((fields, 2 * GROUP * HEAD), BF16),
                pltpu.VMEM((fields, NPAD), F32),
                pltpu.SemaphoreType.DMA((slots // tail, 3)),
                pltpu.SemaphoreType.DMA,
                pltpu.SemaphoreType.DMA((2,)),
                pltpu.SemaphoreType.DMA((groups,)),
                pltpu.SemaphoreType.DMA,
                pltpu.SemaphoreType.REGULAR,
            ],
            compiler_params=pltpu.CompilerParams(
                collective_id=0, has_side_effects=True, vmem_limit_bytes=46 * 1024 * 1024
            ),
            name="synthesis",
        )(*(pltpu.with_memory_space_constraint(v, pltpu.MemorySpace.HBM) for v in (vort, div, leg, wave)), points, cosq)

    both = P(("member", "wave"), None, None)
    return jax.shard_map(
        body,
        mesh=mesh,
        in_specs=(both, both, P("wave", None, None), P(None), P("wave"), P("wave")),
        out_specs=both,
        check_vma=False,
    )
```
